64 devices in a mesh: rep: 8 (over x, y, core), dp: 8 (over z).
Axes of the slice: x: 2, y: 2, z: 8, core: 2. Of those that a mesh axis runs over, the one named last changes fastest.
The devices are a block of a 4x4x8 slice.
Arguments:
- x: bfloat16 [64, 2048, 768], P(('rep', 'dp')), parts along dimension 0
- dy: bfloat16 [64, 2048, 768], P(('rep', 'dp')), parts along dimension 0
- w_gate: bfloat16 [2, 768, 1792], replicated
- w_up: bfloat16 [2, 768, 1792], replicated
- w_down: bfloat16 [2, 1792, 768], replicated
- m_w_gate: float32 [2, 768, 1792], P(None, 'dp')
- m_w_up: float32 [2, 768, 1792], P(None, 'dp')
- m_w_down: float32 [2, 1792, 768], P(None, 'dp')
- v_w_gate: float32 [2, 768, 1792], P(None, 'dp')
- v_w_up: float32 [2, 768, 1792], P(None, 'dp')
- v_w_down: float32 [2, 1792, 768], P(None, 'dp')
Outputs:
- output 1: bfloat16 [16, 768, 1792], P('rep'), parts along dimension 0
- output 2: bfloat16 [16, 768, 1792], P('rep'), parts along dimension 0
- output 3: bfloat16 [16, 1792, 768], P('rep'), parts along dimension 0
- output 4: float32 [16, 768, 1792], P('rep', 'dp'), parts along dimension 0
- output 5: float32 [16, 768, 1792], P('rep', 'dp'), parts along dimension 0
- output 6: float32 [16, 1792, 768], P('rep', 'dp'), parts along dimension 0
- output 7: float32 [16, 768, 1792], P('rep', 'dp'), parts along dimension 0
- output 8: float32 [16, 768, 1792], P('rep', 'dp'), parts along dimension 0
- output 9: float32 [16, 1792, 768], P('rep', 'dp'), parts along dimension 0
There are 8 independent parts. The reference program is written for one: setup_inputs(seed, part) draws one part's arguments, and reference() takes and returns one part's arrays. A program takes and returns all parts, laid end to end along the dimension named above; an argument that names none is the same for every part.
All inputs are finite; a program needn't handle non-finite values.
Results may differ from the reference program's by a relative error of at most 0.022.
Values are sent between devices in bfloat16 or wider.
A program may use at most 768 MiB of HBM per device.

```python
import jax
import jax.numpy as jnp
from jax import lax

SEQUENCES = 8
TOKENS = 2048
D = 768
FF = 1792
LAYERS = 2
NAMES = ("w_gate", "w_up", "w_down")
SHAPES = {"w_gate": (LAYERS, D, FF), "w_up": (LAYERS, D, FF), "w_down": (LAYERS, FF, D)}


def bump(key, n, height):
    away = (jnp.arange(n, dtype=jnp.int32) - jax.random.randint(key, (), 0, n, jnp.int32)) % n
    return jnp.where(away < n // 8, height, 1.0)


def together(key, own, strength):
    shared = jax.random.normal(key, own.shape[1:], jnp.float32)
    return (own + strength * shared) * lax.rsqrt(1 + strength * strength)


def setup_inputs(seed: int = 0, part: int = 0) -> dict:
    kx, kdy, ka, kb, kz, kf, kh, kl, *keys = jax.random.split(jax.random.key(seed), 8 + 3 * len(NAMES))
    kx, kdy, ka, kb = (jax.random.fold_in(k, part) for k in (kx, kdy, ka, kb))
    kw, km, kv = (keys[i::3] for i in range(3))
    shape = (SEQUENCES, TOKENS, D)
    much_x, much_dy = jax.random.uniform(kz, (2,), jnp.float32, 0.0, 1.0)
    loud = 2.0 ** jax.random.uniform(jax.random.fold_in(kz, 1), (), jnp.float32, -1.0, 2.0)
    layers = 2.0 ** jax.random.uniform(kl, (LAYERS, 1, 1), jnp.float32, -1.0, 1.0)
    x = together(ka, jax.random.normal(kx, shape, jnp.float32), much_x) * bump(kf, D, 4.0)
    dy = together(kb, jax.random.normal(kdy, shape, jnp.float32), much_dy)
    drawn = {"x": x.astype(jnp.bfloat16), "dy": (loud * dy * (SEQUENCES * TOKENS) ** -0.5).astype(jnp.bfloat16)}
    for key, name in zip(kw, NAMES, strict=True):
        w = jax.random.normal(key, SHAPES[name], jnp.float32) * SHAPES[name][1] ** -0.5
        drawn[name] = (w * {"w_gate": 1.0, "w_up": bump(kh, FF, 4.0), "w_down": layers}[name]).astype(jnp.bfloat16)
    for key, name in zip(km, NAMES, strict=True):
        drawn[f"m_{name}"] = 0.1 * jax.random.normal(key, SHAPES[name], jnp.float32)
    for key, name in zip(kv, NAMES, strict=True):
        drawn[f"v_{name}"] = jax.random.uniform(key, SHAPES[name], jnp.float32, 0.005, 0.015)
    return drawn


def matmul(a, w):
    return jnp.dot(a, w, preferred_element_type=jnp.float32).astype(jnp.bfloat16)


def normed(h):
    wide = h.astype(jnp.float32)
    scale = lax.rsqrt(jnp.mean(wide**2, -1, keepdims=True) + 1e-6)
    return (wide * scale).astype(jnp.bfloat16)


def layer(h, w):
    a = normed(h)
    gate = jnp.dot(a, w["w_gate"], preferred_element_type=jnp.float32)
    up = jnp.dot(a, w["w_up"], preferred_element_type=jnp.float32)
    return h + matmul((jax.nn.silu(gate) * up).astype(jnp.bfloat16), w["w_down"])


def adamw(w, m, v, g):
    m = 0.9 * m + 0.1 * g
    v = 0.95 * v + 0.05 * g * g
    step = m * lax.rsqrt(v + 1e-8) + 0.1 * w
    return (w - 0.02 * step).astype(jnp.bfloat16), m, v


def clipped(gradients, sum_of_squares, count):
    factor = jnp.minimum(1.0, 0.5 * lax.rsqrt(sum_of_squares / count + 1e-30))
    return [g * factor for g in gradients]


def stack(weights, h):
    return lax.scan(lambda h, w: (layer(h, w), None), h, weights)[0]


def reference(x, dy, w_gate, w_up, w_down, m_w_gate, m_w_up, m_w_down, v_w_gate, v_w_up, v_w_down):
    weights = dict(zip(NAMES, (w_gate, w_up, w_down), strict=True))

    def take(so_far, sequence):
        h, by_y = sequence
        _, back = jax.vjp(lambda w: stack(w, h), weights)
        return jax.tree.map(lambda total, term: total + term.astype(jnp.float32), so_far, back(by_y)[0]), None

    none_yet = {name: jnp.zeros(w.shape, jnp.float32) for name, w in weights.items()}
    by_weights, _ = lax.scan(take, none_yet, (x, dy))
    gradients = [by_weights[name].astype(jnp.bfloat16).astype(jnp.float32) for name in NAMES]
    gradients = clipped(gradients, sum(jnp.sum(g * g) for g in gradients), sum(g.size for g in gradients))
    new = [
        adamw(w.astype(jnp.float32), m, v, g)
        for w, m, v, g in zip((w_gate, w_up, w_down), (m_w_gate, m_w_up, m_w_down), (v_w_gate, v_w_up, v_w_down), gradients, strict=True)
    ]
    return tuple(one[which] for which in range(3) for one in new)
```

```python
import functools

import jax
import jax.numpy as jnp
from jax import lax
from jax.experimental import pallas as pl
from jax.experimental.pallas import tpu as pltpu
from jax.sharding import PartitionSpec as P

NAMES = ("w_gate", "w_up", "w_down")
MESH = pl.DeviceIdType.MESH
F32, BF16 = jnp.float32, jnp.bfloat16
COLS = 256
VMEM_MAX = 67_043_328


def matmul(a, w):
    return jnp.dot(a, w, preferred_element_type=jnp.float32).astype(jnp.bfloat16)


def normed(h):
    wide = h.astype(jnp.float32)
    scale = lax.rsqrt(jnp.mean(wide**2, -1, keepdims=True) + 1e-6)
    return (wide * scale).astype(jnp.bfloat16)


def layer(h, w):
    a = normed(h)
    gate = jnp.dot(a, w["w_gate"], preferred_element_type=jnp.float32)
    up = jnp.dot(a, w["w_up"], preferred_element_type=jnp.float32)
    return h + matmul((jax.nn.silu(gate) * up).astype(jnp.bfloat16), w["w_down"])


def stack(weights, h):
    for number in range(weights["w_gate"].shape[0]):
        h = layer(h, {name: w[number] for name, w in weights.items()})
    return h


class Plan:
    def __init__(self, n, layers, d, ff):
        self.n, self.layers, self.d, self.ff = n, layers, d, ff
        self.rows = d // n
        self.block = ff // n
        self.wide = d // COLS
        self.strip = self.rows // self.wide
        self.chunks = ff // COLS
        self.strips = self.block // self.strip
        self.hops = n // 2
        assert n % 2 == 0 and d % COLS == 0 and ff % COLS == 0 and self.rows % (16 * self.wide) == 0
        assert self.block % self.strip == 0
        subs = []
        late = []
        for l in reversed(range(layers)):
            for c in range(self.chunks):
                subs += [("gate", l, c), ("up", l, c)]
            downs = late + [("down", l, s) for s in range(self.strips)]
            late = downs[len(downs) // 2 * 2 :]
            subs += downs[: len(downs) // 2 * 2]
        assert not late
        self.subs = subs
        self.units = len(subs) // 2

    def each(self):
        for i, (kind, l, k) in enumerate(self.subs):
            yield i // 2, i % 2, kind, l, k

    def views(self, p, half, kind, l, k, own, arrays, lead=()):
        gate, up, down = arrays
        if kind != "down":
            array = gate if kind == "gate" else up
            yield own.at[(p, *lead, half)], array.at[(l, *lead, slice(None), pl.ds(k * COLS, COLS))]
        else:
            for c in range(self.wide):
                yield (
                    own.at[(p, *lead, half, pl.ds(c * self.strip, self.strip))],
                    down.at[(l, *lead, pl.ds(k * self.strip, self.strip), pl.ds(c * COLS, COLS))],
                )


def comm_kernel(plan, count, grads, weights, moments_m, moments_v, own, m, v, landing, w, squares, sums, local_sems, send, recv, send_s, recv_s):
    n, hops, units = plan.n, plan.hops, plan.units
    me = lax.axis_index("dp")
    right, left = lax.rem(me + 1, n), lax.rem(me + n - 1, n)

    def at(k):
        return lax.rem(me + k + n, n)

    barrier = pltpu.get_barrier_semaphore()
    for k in range(1, n):
        pl.semaphore_signal(barrier, inc=1, device_id={"dp": at(k)}, device_id_type=MESH)

    every = slice(None)
    for p, half, kind, l, k in plan.each():
        for inside, outside in plan.views(p, half, kind, l, k, own, grads, (every,)):
            pltpu.make_async_copy(outside, inside, local_sems.at[0]).start()
    for p, half, kind, l, k in plan.each():
        for inside, outside in plan.views(p, half, kind, l, k, w, [a.at[:, me] for a in weights]):
            pltpu.make_async_copy(outside, inside, local_sems.at[1]).start()
        for inside, outside in plan.views(p, half, kind, l, k, m, moments_m):
            pltpu.make_async_copy(outside, inside, local_sems.at[2]).start()
        for inside, outside in plan.views(p, half, kind, l, k, v, moments_v):
            pltpu.make_async_copy(outside, inside, local_sems.at[3]).start()
    pl.semaphore_wait(barrier, n - 1)
    pltpu.make_async_copy(own, own, local_sems.at[0]).wait()

    def hop(p, h, d):
        b = at(hops - h) if d == 0 else at(h - hops)
        if h == 0:
            source, target = own.at[p, b, d], landing.at[p, d, 0, d]
        else:
            source, target = own.at[p, b], landing.at[p, d, h]
        return pltpu.make_async_remote_copy(
            source, target, send.at[p, h, d], recv.at[p, h, d], device_id={"dp": right if d == 0 else left}, device_id_type=MESH
        )

    for h in range(hops):

        @pl.loop(0, units)
        def _(p, h=h):
            for d in (0, 1):
                if h > 0:
                    hop(p, h - 1, d).wait_recv()
                    b = at(hops - h) if d == 0 else at(h - hops)
                    if h == 1:
                        own[p, b, d] = (own[p, b, d].astype(F32) + landing[p, d, 0, d].astype(F32)).astype(BF16)
                    else:
                        own[p, b] = (own[p, b].astype(F32) + landing[p, d, h - 1].astype(F32)).astype(BF16)
                hop(p, h, d).start()

    squares[...] = jnp.zeros_like(squares)

    @pl.loop(0, units)
    def _(p):
        for d in (0, 1):
            hop(p, hops - 1, d).wait_recv()
        for half in (0, 1):
            g = own[p, me, half].astype(F32) + landing[p, 0, hops - 1, half].astype(F32) + landing[p, 1, hops - 1, half].astype(F32)
            g = g.astype(BF16)
            own[p, me, half] = g
            g = g.astype(F32)
            squares[...] += g * g
        for h in range(hops):
            for d in (0, 1):
                hop(p, h, d).wait_send()

    part = jnp.sum(squares[...].reshape(-1, 8, COLS), axis=0)
    part = sum(part[:, i * 128 : (i + 1) * 128] for i in range(COLS // 128))
    sums[0] = part

    def tell(k):
        return pltpu.make_async_remote_copy(
            sums.at[0], sums.at[k], send_s.at[k], recv_s.at[k], device_id={"dp": at(k)}, device_id_type=MESH
        )

    for k in range(1, n):
        tell(k).start()
    pltpu.make_async_copy(w, w, local_sems.at[1]).wait()
    pltpu.make_async_copy(m, m, local_sems.at[2]).wait()
    pltpu.make_async_copy(v, v, local_sems.at[3]).wait()
    for k in range(1, n):
        tell(k).wait_recv()
    total = jnp.sum(jnp.sum(sums[...], axis=0), axis=(0, 1), keepdims=True)
    factor = jnp.minimum(1.0, 0.5 * lax.rsqrt(total / count + 1e-30))
    for k in range(1, n):
        tell(k).wait_send()

    def pass_on(p, h, d):
        b = at(-h) if d == 0 else at(h)
        ref = own.at[p, b] if h < hops - 1 else own.at[p, b, d]
        return pltpu.make_async_remote_copy(
            ref, ref, send.at[p, h, d], recv.at[p, h, d], device_id={"dp": right if d == 0 else left}, device_id_type=MESH
        )

    @pl.loop(0, units)
    def _(p):
        for half in (0, 1):
            g = own[p, me, half].astype(F32) * factor
            new_m = 0.9 * m[p, half] + 0.1 * g
            new_v = 0.95 * v[p, half] + 0.05 * g * g
            old = w[p, half].astype(F32)
            step = new_m * lax.rsqrt(new_v + 1e-8) + 0.1 * old
            own[p, me, half] = (old - 0.02 * step).astype(BF16)
            m[p, half] = new_m
            v[p, half] = new_v
        for d in (0, 1):
            pass_on(p, 0, d).start()

    for h in range(1, hops):

        @pl.loop(0, units)
        def _(p, h=h):
            for d in (0, 1):
                pass_on(p, h - 1, d).wait_recv()
                pass_on(p, h, d).start()

    @pl.loop(0, units)
    def _(p):
        for d in (0, 1):
            pass_on(p, hops - 1, d).wait_recv()
            for h in range(hops):
                pass_on(p, h, d).wait_send()


def place_kernel(plan, own, m, v, weights, new_m, new_v, sems):
    every = slice(None)
    copies = []
    for p, half, kind, l, k in plan.each():
        for inside, outside in plan.views(p, half, kind, l, k, own, weights, (every,)):
            copies.append((inside, outside, 0))
        for inside, outside in plan.views(p, half, kind, l, k, m, new_m):
            copies.append((inside, outside, 1))
        for inside, outside in plan.views(p, half, kind, l, k, v, new_v):
            copies.append((inside, outside, 2))
    for inside, outside, s in copies:
        pltpu.make_async_copy(inside, outside, sems.at[s]).start()
    for inside, outside, s in copies:
        pltpu.make_async_copy(inside, outside, sems.at[s]).wait()


def solution(mesh):
    n = mesh.shape["dp"]

    def step(x, dy, *arrays):
        weights, m, v = (arrays[i : i + 3] for i in (0, 3, 6))
        layers, d, ff = weights[0].shape
        plan = Plan(n, layers, d, ff)
        _, back = jax.vjp(lambda w: stack(w, x[0]), dict(zip(NAMES, weights, strict=True)))
        by_weights = back(dy[0])[0]
        grads = [by_weights[name].reshape(layers, n, -1, by_weights[name].shape[-1]) for name in NAMES]
        blocks = [w.reshape(layers, n, -1, w.shape[-1]) for w in weights]
        count = float(sum(w.size for w in weights))
        units, rows = plan.units, plan.rows
        anywhere = pl.BlockSpec(memory_space=pl.ANY)

        def body(*refs):
            grads, weights, m, v = (refs[i : i + 3] for i in (0, 3, 6, 9))
            comm_kernel(plan, count, grads, weights, m, v, *refs[12:])

        out_shape = [
            pltpu.VMEM((units, n, 2, rows, COLS), BF16),
            pltpu.VMEM((units, 2, rows, COLS), F32),
            pltpu.VMEM((units, 2, rows, COLS), F32),
        ]
        own, new_m, new_v = pl.pallas_call(
            body,
            out_shape=out_shape,
            in_specs=[anywhere] * 12,
            out_specs=[pl.BlockSpec(memory_space=pltpu.VMEM)] * 3,
            scratch_shapes=[
                pltpu.VMEM((units, 2, plan.hops, 2, rows, COLS), BF16),
                pltpu.VMEM((units, 2, rows, COLS), BF16),
                pltpu.VMEM((rows, COLS), F32),
                pltpu.VMEM((n, 8, 128), F32),
                pltpu.SemaphoreType.DMA((4,)),
                pltpu.SemaphoreType.DMA((units, plan.hops, 2)),
                pltpu.SemaphoreType.DMA((units, plan.hops, 2)),
                pltpu.SemaphoreType.DMA((n,)),
                pltpu.SemaphoreType.DMA((n,)),
            ],
            compiler_params=pltpu.CompilerParams(collective_id=0, has_side_effects=True, vmem_limit_bytes=24 * 2**20),
            name="exchange",
        )(*grads, *blocks, *m, *v)

        def place(*refs):
            place_kernel(plan, *refs[:3], refs[3:6], refs[6:9], refs[9:12], refs[12])

        shapes = [jax.ShapeDtypeStruct(b.shape, b.dtype) for b in blocks]
        shapes += [jax.ShapeDtypeStruct(t.shape, t.dtype) for t in (*m, *v)]
        out = pl.pallas_call(
            place,
            out_shape=shapes,
            in_specs=[pl.BlockSpec(memory_space=pltpu.VMEM)] * 3,
            out_specs=[anywhere] * 9,
            scratch_shapes=[pltpu.SemaphoreType.DMA((3,))],
            compiler_params=pltpu.CompilerParams(vmem_limit_bytes=2**20),
            name="place",
        )(own, new_m, new_v)
        return tuple(o.reshape(w.shape) for o, w in zip(out[:3], weights)) + tuple(out[3:])

    rows = P(None, "dp", None)
    seq = P(("rep", "dp"), None, None)
    return jax.shard_map(
        step,
        mesh=mesh,
        in_specs=(seq, seq, P(), P(), P()) + (rows,) * 6,
        out_specs=(P("rep"),) * 3 + (P("rep", "dp", None),) * 6,
        check_vma=False,
    )
```

```python
import jax
import jax.numpy as jnp
from jax import lax
from jax.experimental import pallas as pl
from jax.experimental.pallas import tpu as pltpu
from jax.sharding import PartitionSpec as P

MESH = pl.DeviceIdType.MESH
F32, BF16 = jnp.float32, jnp.bfloat16
COLS = 256
TILE = 512
VMEM = 67_043_328
EVERY = slice(None)


def dot(a, b, contract=(1, 0)):
    return lax.dot_general(a, b, (((contract[0],), (contract[1],)), ((), ())), preferred_element_type=F32)


def normed(h):
    wide = h.astype(F32)
    return (wide * lax.rsqrt(jnp.mean(wide * wide, -1, keepdims=True) + 1e-6)).astype(BF16)


def sigmoid(x):
    return 0.5 * jnp.tanh(0.5 * x) + 0.5


class Plan:
    def __init__(self, n, tokens, layers, d, ff):
        self.n, self.tokens, self.layers, self.d, self.ff = n, tokens, layers, d, ff
        self.rows, self.block = d // n, ff // n
        self.folds, self.chunks = d // COLS, ff // COLS
        self.strip = self.rows // self.folds
        self.strips = self.block // self.strip
        self.hops = n // 2
        assert layers == 2 and n % 2 == 0 and d % COLS == 0 and ff % COLS == 0 and tokens % TILE == 0
        assert self.rows % (16 * self.folds) == 0 and self.block % self.strip == 0 and COLS % self.strip == 0
        self.subs, late = [], []
        for l in reversed(range(layers)):
            for c in range(self.chunks):
                self.subs += [("gate", l, c), ("up", l, c)]
            late += [("down", l, s) for s in range(self.strips)]
            even = len(late) // 2 * 2
            self.subs, late = self.subs + late[:even], late[even:]
        assert not late
        self.units = len(self.subs) // 2
        self.at = {sub: i for i, sub in enumerate(self.subs)}

    def down_sub(self, l, s):
        first = self.at["down", l, 0]
        steps = [self.at["down", l, k] - self.at["down", l, k - 1] - 1 for k in range(1, self.strips)]
        place = first + s
        for k, extra in enumerate(steps, 1):
            if extra:
                place += lax.div(s + (self.strips - k), self.strips) * extra
        return place

    def views(self, i, own, arrays, lead=()):
        kind, l, k = self.subs[i]
        gate, up, down = arrays
        if kind != "down":
            yield own(i, pl.ds(0, self.rows)), (gate if kind == "gate" else up).at[(l, *lead, EVERY, pl.ds(k * COLS, COLS))]
        else:
            for f in range(self.folds):
                yield (
                    own(i, pl.ds(f * self.strip, self.strip)),
                    down.at[(l, *lead, pl.ds(k * self.strip, self.strip), pl.ds(f * COLS, COLS))],
                )


def flat(ref, rows, first=0):
    return lambda i, part: ref.at[pl.ds((first + i) * rows + part.start, part.size)]


def step_kernel(plan, count, x, dy, weights, blocks, moments_m, moments_v, own, mv, *scratch):
    (x_buf, a, dh, h1, sdd, gate_buf, up_buf, down_buf, half_landing, landing, squares, sums) = scratch[:12]
    (in_sems, weight_sems, state_sems, send, recv, tell_send, tell_recv) = scratch[12:]
    n, hops, units, chunks, rows, tokens = plan.n, plan.hops, plan.units, plan.chunks, plan.rows, plan.tokens
    me = lax.axis_index("dp")
    right, left = lax.rem(me + 1, n), lax.rem(me + n - 1, n)

    def at(k):
        return lax.rem(me + k + n, n)

    barrier = pltpu.get_barrier_semaphore()
    for k in range(1, n):
        pl.semaphore_signal(barrier, inc=1, device_id={"dp": at(k)}, device_id_type=MESH)

    s_, dg_, du_ = (sdd.at[pl.ds(i * tokens, tokens)] for i in range(3))
    acc = mv
    tiles = [pl.ds(t, TILE) for t in range(0, tokens, TILE)]

    def part(f, t):
        return pl.ds(f * tokens + t.start, TILE)

    passes = (0, 1, 0)

    def weight_copies(l, c, slot):
        chunk = pl.ds(pl.multiple_of(c * COLS, COLS), COLS)
        for i, (source, target) in enumerate(
            ((weights[0].at[l, :, chunk], gate_buf), (weights[1].at[l, :, chunk], up_buf), (weights[2].at[l, chunk], down_buf))
        ):
            yield pltpu.make_async_copy(source, target.at[slot], weight_sems.at[i, slot])

    def begin(k, c):
        slot = lax.rem(k * chunks + c, 2)
        for copy in weight_copies(passes[k], c, slot):
            copy.wait()

        @pl.when(c + 1 < chunks)
        def _():
            for copy in weight_copies(passes[k], c + 1, 1 - slot):
                copy.start()

        if k + 1 < len(passes):

            @pl.when(c + 1 == chunks)
            def _():
                for copy in weight_copies(passes[k + 1], 0, 1 - slot):
                    copy.start()

        return slot

    def add_to_acc(t, value):
        for f in range(plan.folds):
            acc[part(f, t)] += value[:, f * COLS : (f + 1) * COLS]

    def clear_acc():
        for f in range(plan.folds):
            acc[pl.ds(f * tokens, tokens)] = jnp.zeros((tokens, COLS), F32)

    def read_acc(t):
        return jnp.concatenate([acc[part(f, t)] for f in range(plan.folds)], axis=1).astype(BF16).astype(F32)

    load_x = pltpu.make_async_copy(x, x_buf, in_sems.at[0])
    load_dy = pltpu.make_async_copy(dy, dh, in_sems.at[1])
    load_x.start()
    for copy in weight_copies(0, 0, 0):
        copy.start()
    load_dy.start()
    load_x.wait()

    clear_acc()
    for t in tiles:
        a[t] = normed(x_buf[t])

    @pl.loop(0, chunks)
    def _(c):
        slot = begin(0, c)
        for t in tiles:
            gate, up = dot(a[t], gate_buf[slot]), dot(a[t], up_buf[slot])
            add_to_acc(t, dot((gate * sigmoid(gate) * up).astype(BF16), down_buf[slot]))

    for t in tiles:
        h = (x_buf[t].astype(F32) + read_acc(t)).astype(BF16)
        h1[t] = h
        a[t] = normed(h)
    clear_acc()
    load_dy.wait()

    def hop(p, h, d):
        b = at(hops - h) if d == 0 else at(h - hops)
        if h == 0:
            source, target = own.at[p, b, d], half_landing.at[p, d]
        else:
            source, target = own.at[p, b], landing.at[p, d, h - 1]
        return pltpu.make_async_remote_copy(
            source, target, send.at[p, h, d], recv.at[p, h, d], device_id={"dp": right if d == 0 else left}, device_id_type=MESH
        )

    def advance(p, h):
        for d in (0, 1):
            if h > 0:
                hop(p, h - 1, d).wait_recv()
                b = at(hops - h) if d == 0 else at(h - hops)
                if h == 1:
                    own[p, b, d] = (own[p, b, d].astype(F32) + half_landing[p, d].astype(F32)).astype(BF16)
                else:
                    own[p, b] = (own[p, b].astype(F32) + landing[p, d, h - 2].astype(F32)).astype(BF16)
            hop(p, h, d).start()

    def finish(p):
        for d in (0, 1):
            hop(p, hops - 1, d).wait_recv()
        for half in (0, 1):
            g = own[p, me, half].astype(F32) + landing[p, 0, hops - 2, half].astype(F32) + landing[p, 1, hops - 2, half].astype(F32)
            g = g.astype(BF16)
            own[p, me, half] = g
            g = g.astype(F32)
            squares[...] += g * g

    def serve(t):
        for h in range(hops):

            @pl.when(jnp.logical_and(t - h >= 0, t - h < units))
            def _(h=h):
                advance(t - h, h)

        @pl.when(jnp.logical_and(t - hops >= 0, t - hops < units))
        def _():
            finish(t - hops)

    def chunk_gradients(k, c, first, serve_now):
        l = passes[k]
        slot = begin(k, c)
        for t in tiles:
            gate, up = dot(a[t], gate_buf[slot]), dot(a[t], up_buf[slot])
            ds = dot(dh[t], down_buf[slot], (1, 1)).astype(BF16).astype(F32)
            sig = sigmoid(gate)
            silu = gate * sig
            s_[t] = (silu * up).astype(BF16)
            du_[t] = (ds * silu).astype(BF16)
            dg_[t] = (ds * up * (sig + silu * (1.0 - sig))).astype(BF16)
        for half, by in ((0, dg_), (1, du_)):
            own[first + c, :, half] = dot(a[...], by[...], (0, 0)).astype(BF16).reshape(n, rows, COLS)
        serve_now()
        by_down = dot(s_[...], dh[...], (0, 0)).astype(BF16)
        for g in range(COLS // plan.strip):
            group = c * (COLS // plan.strip) + g
            b, s = lax.div(group, plan.strips), lax.rem(group, plan.strips)
            i = plan.down_sub(l, s)
            for f in range(plan.folds):
                own[lax.div(i, 2), b, lax.rem(i, 2), f * plan.strip : (f + 1) * plan.strip] = by_down[
                    g * plan.strip : (g + 1) * plan.strip, f * COLS : (f + 1) * COLS
                ]
        return slot

    pl.semaphore_wait(barrier, n - 1)
    squares[...] = jnp.zeros_like(squares)

    @pl.loop(0, chunks)
    def _(c):
        slot = chunk_gradients(1, c, plan.at["gate", 1, 0] // 2, lambda: serve(c))
        for t in tiles:
            add_to_acc(t, dot(dg_[t], gate_buf[slot], (1, 1)) + dot(du_[t], up_buf[slot], (1, 1)))

    for t in tiles:
        h, da = h1[t].astype(F32), read_acc(t)
        scale = lax.rsqrt(jnp.mean(h * h, -1, keepdims=True) + 1e-6)
        by_norm = scale * da - h * (scale * scale * scale * jnp.mean(da * h, -1, keepdims=True))
        dh[t] = (dh[t].astype(F32) + by_norm.astype(BF16).astype(F32)).astype(BF16)
        a[t] = normed(x_buf[t])

    @pl.loop(0, chunks)
    def _(c):
        chunk_gradients(2, c, plan.at["gate", 0, 0] // 2, lambda: serve(chunks + c))

    w_block, m_block, v_block = flat(sdd, rows), flat(mv, rows), flat(mv, rows, len(plan.subs))
    held = len(plan.subs) * rows
    for s, (block, arrays) in enumerate(((w_block, [b.at[:, me] for b in blocks]), (m_block, moments_m), (v_block, moments_v))):
        for i in range(len(plan.subs)):
            for inside, outside in plan.views(i, block, arrays):
                pltpu.make_async_copy(outside, inside, state_sems.at[s]).start()

    @pl.loop(2 * chunks, units + hops)
    def _(t):
        serve(t)

    @pl.loop(0, units)
    def _(p):
        for h in range(hops):
            for d in (0, 1):
                hop(p, h, d).wait_send()

    folded = jnp.sum(squares[...].reshape(-1, 8, COLS), axis=0)
    sums[0] = sum(folded[:, i : i + 128] for i in range(0, COLS, 128))

    def tell(k):
        return pltpu.make_async_remote_copy(
            sums.at[0], sums.at[k], tell_send.at[k], tell_recv.at[k], device_id={"dp": at(k)}, device_id_type=MESH
        )

    for k in range(1, n):
        tell(k).start()
    for s, ref in enumerate((sdd.at[pl.ds(0, held)], mv.at[pl.ds(0, held)], mv.at[pl.ds(held, held)])):
        pltpu.make_async_copy(ref, ref, state_sems.at[s]).wait()
    for k in range(1, n):
        tell(k).wait_recv()
    total = jnp.sum(jnp.sum(sums[...], axis=0), axis=(0, 1), keepdims=True)
    factor = jnp.minimum(1.0, 0.5 * lax.rsqrt(total / count + 1e-30))
    for k in range(1, n):
        tell(k).wait_send()

    def pass_on(p, h, d):
        b = at(-h) if d == 0 else at(h)
        ref = own.at[p, b] if h < hops - 1 else own.at[p, b, d]
        return pltpu.make_async_remote_copy(
            ref, ref, send.at[p, h, d], recv.at[p, h, d], device_id={"dp": right if d == 0 else left}, device_id_type=MESH
        )

    @pl.loop(0, units)
    def _(p):
        for half in (0, 1):
            start = pl.multiple_of((2 * p + half) * rows, rows)
            here, there = pl.ds(start, rows), pl.ds(start + held, rows)
            g = own[p, me, half].astype(F32) * factor
            m = 0.9 * mv[here] + 0.1 * g
            v = 0.95 * mv[there] + 0.05 * g * g
            w = sdd[here].astype(F32)
            own[p, me, half] = (w - 0.02 * (m * lax.rsqrt(v + 1e-8) + 0.1 * w)).astype(BF16)
            mv[here] = m
            mv[there] = v
        for d in (0, 1):
            pass_on(p, 0, d).start()

    for h in range(1, hops):

        @pl.loop(0, units)
        def _(p, h=h):
            for d in (0, 1):
                pass_on(p, h - 1, d).wait_recv()
                pass_on(p, h, d).start()

    @pl.loop(0, units)
    def _(p):
        for d in (0, 1):
            pass_on(p, hops - 1, d).wait_recv()
            for h in range(hops):
                pass_on(p, h, d).wait_send()


def place_kernel(plan, own, mv, weights, new_m, new_v, sems):
    def gathered(i, part):
        return own.at[i // 2, :, i % 2, part]

    copies = []
    for i in range(len(plan.subs)):
        for s, (block, arrays, lead) in enumerate(
            (
                (gathered, weights, (EVERY,)),
                (flat(mv, plan.rows), new_m, ()),
                (flat(mv, plan.rows, len(plan.subs)), new_v, ()),
            )
        ):
            copies += [pltpu.make_async_copy(*views, sems.at[s]) for views in plan.views(i, block, arrays, lead)]
    for copy in copies:
        copy.start()
    for copy in copies:
        copy.wait()


def solution(mesh):
    n = mesh.shape["dp"]

    def step(x, dy, *arrays):
        weights, m, v = (arrays[i : i + 3] for i in (0, 3, 6))
        layers, d, ff = weights[0].shape
        tokens = x.shape[1]
        plan = Plan(n, tokens, layers, d, ff)
        blocks = [w.reshape(layers, n, -1, w.shape[-1]) for w in weights]
        count = float(sum(w.size for w in weights))
        units, rows, hops, subs = plan.units, plan.rows, plan.hops, len(plan.subs)
        anywhere, in_vmem = pl.BlockSpec(memory_space=pl.ANY), pl.BlockSpec(memory_space=pltpu.VMEM)

        def body(x, dy, *refs):
            weights, blocks, m, v = (refs[i : i + 3] for i in (0, 3, 6, 9))
            step_kernel(plan, count, x, dy, weights, blocks, m, v, *refs[12:])

        results = [pltpu.VMEM((units, n, 2, rows, COLS), BF16), pltpu.VMEM((2 * subs * rows, COLS), F32)]
        own, mv = pl.pallas_call(
            body,
            out_shape=results,
            in_specs=[anywhere] * 14,
            out_specs=[in_vmem] * 2,
            scratch_shapes=[pltpu.VMEM((tokens, d), BF16)] * 4
            + [
                pltpu.VMEM((3 * tokens, COLS), BF16),
                pltpu.VMEM((2, d, COLS), BF16),
                pltpu.VMEM((2, d, COLS), BF16),
                pltpu.VMEM((2, COLS, d), BF16),
                pltpu.VMEM((units, 2, rows, COLS), BF16),
                pltpu.VMEM((units, 2, hops - 1, 2, rows, COLS), BF16),
                pltpu.VMEM((rows, COLS), F32),
                pltpu.VMEM((n, 8, 128), F32),
                pltpu.SemaphoreType.DMA((2,)),
                pltpu.SemaphoreType.DMA((3, 2)),
                pltpu.SemaphoreType.DMA((3,)),
                pltpu.SemaphoreType.DMA((units, hops, 2)),
                pltpu.SemaphoreType.DMA((units, hops, 2)),
                pltpu.SemaphoreType.DMA((n,)),
                pltpu.SemaphoreType.DMA((n,)),
            ],
            compiler_params=pltpu.CompilerParams(collective_id=0, has_side_effects=True, vmem_limit_bytes=38 * 2**20),
            name="step",
        )(x[0], dy[0], *weights, *blocks, *m, *v)

        def place(*refs):
            place_kernel(plan, *refs[:2], refs[2:5], refs[5:8], refs[8:11], refs[11])

        out = pl.pallas_call(
            place,
            out_shape=[jax.ShapeDtypeStruct(t.shape, t.dtype) for t in (*blocks, *m, *v)],
            in_specs=[in_vmem] * 2,
            out_specs=[anywhere] * 9,
            scratch_shapes=[pltpu.SemaphoreType.DMA((3,))],
            compiler_params=pltpu.CompilerParams(vmem_limit_bytes=2**20),
            name="place",
        )(own, mv)
        return tuple(o.reshape(w.shape) for o, w in zip(out[:3], weights)) + tuple(out[3:])

    block = P(None, "dp", None)
    sequence = P(("rep", "dp"), None, None)
    return jax.shard_map(
        step,
        mesh=mesh,
        in_specs=(sequence, sequence, P(), P(), P()) + (block,) * 6,
        out_specs=(P("rep"),) * 3 + (P("rep", "dp", None),) * 6,
        check_vma=False,
    )
```

```python
import jax
import jax.numpy as jnp
from jax import lax
from jax.experimental import pallas as pl
from jax.experimental.pallas import tpu as pltpu
from jax.sharding import PartitionSpec as P

MESH = pl.DeviceIdType.MESH
F32, BF16 = jnp.float32, jnp.bfloat16
COLS = 256
TILE = 512
VMEM = 67_043_328
EVERY = slice(None)
LATE = 99
HOPS = (
    (2, 5, 7, 11, 13, 16, 20, 20, 20, 21, 32, 34, 36, 39, 42, 46, *(LATE,) * 5),
    (3, 6, 10, 13, 15, 19, 23, 24, 25, 25, 34, 35, 38, 42, 44, 48, *(LATE,) * 5),
    (6, 8, 12, 16, 17, 21, 27, 27, 29, 33, 36, 38, 40, 44, 46, *(LATE,) * 6),
    (9, 11, 15, 22, 24, 28, 29, 31, 31, 37, 40, 43, 45, 46, 49, *(LATE,) * 6),
    (13, 15, 19, 26, 28, 32, 33, 35, 35, 41, 44, 47, 49, *(LATE,) * 8),
)


def dot(a, b, contract=(1, 0)):
    return lax.dot_general(a, b, (((contract[0],), (contract[1],)), ((), ())), preferred_element_type=F32)


def normed(h):
    wide = h.astype(F32)
    return (wide * lax.rsqrt(jnp.mean(wide * wide, -1, keepdims=True) + 1e-6)).astype(BF16)


def sigmoid(x):
    return 0.5 * jnp.tanh(0.5 * x) + 0.5


class Plan:
    def __init__(self, n, tokens, layers, d, ff):
        self.n, self.tokens, self.layers, self.d, self.ff = n, tokens, layers, d, ff
        self.rows, self.block = d // n, ff // n
        self.folds, self.chunks = d // COLS, ff // COLS
        self.strip = self.rows // self.folds
        self.strips = self.block // self.strip
        self.hops = n // 2
        assert layers == 2 and n % 2 == 0 and d % COLS == 0 and ff % COLS == 0 and tokens % TILE == 0
        assert self.rows % (16 * self.folds) == 0 and self.block % self.strip == 0 and COLS % self.strip == 0
        self.subs, late = [], []
        for l in reversed(range(layers)):
            for c in range(self.chunks):
                self.subs += [("gate", l, c), ("up", l, c)]
            late += [("down", l, s) for s in range(self.strips)]
            even = len(late) // 2 * 2
            self.subs, late = self.subs + late[:even], late[even:]
        assert not late
        self.units = len(self.subs) // 2
        assert self.hops + 1 == len(HOPS) and all(len(h) == self.units for h in HOPS)
        self.at = {sub: i for i, sub in enumerate(self.subs)}

    def down_sub(self, l, s):
        first = self.at["down", l, 0]
        steps = [self.at["down", l, k] - self.at["down", l, k - 1] - 1 for k in range(1, self.strips)]
        place = first + s
        for k, extra in enumerate(steps, 1):
            if extra:
                place += lax.div(s + (self.strips - k), self.strips) * extra
        return place

    def views(self, i, own, arrays, lead=()):
        kind, l, k = self.subs[i]
        gate, up, down = arrays
        if kind != "down":
            yield own(i, pl.ds(0, self.rows)), (gate if kind == "gate" else up).at[(l, *lead, EVERY, pl.ds(k * COLS, COLS))]
        else:
            for f in range(self.folds):
                yield (
                    own(i, pl.ds(f * self.strip, self.strip)),
                    down.at[(l, *lead, pl.ds(k * self.strip, self.strip), pl.ds(f * COLS, COLS))],
                )


def flat(ref, rows, first=0):
    return lambda i, part: ref.at[pl.ds((first + i) * rows + part.start, part.size)]


def step_kernel(plan, count, x, dy, weights, blocks, moments_m, moments_v, own, mv, stash, *scratch):
    (x_buf, a, dh, sdd, gate_buf, up_buf, down_buf, half_landing, landing, squares, sums) = scratch[:11]
    (in_sems, weight_sems, stash_sems, state_sems, send, recv, tell_send, tell_recv) = scratch[11:]
    n, hops, units, chunks, rows, tokens = plan.n, plan.hops, plan.units, plan.chunks, plan.rows, plan.tokens
    me = lax.axis_index("dp")
    right, left = lax.rem(me + 1, n), lax.rem(me + n - 1, n)

    def at(k):
        return lax.rem(me + k + n, n)

    barrier = pltpu.get_barrier_semaphore()
    for k in range(1, n):
        pl.semaphore_signal(barrier, inc=1, device_id={"dp": at(k)}, device_id_type=MESH)

    s_, dg_, du_ = (sdd.at[pl.ds(i * tokens, tokens)] for i in (0, 2, 3))
    pairs = [sdd.at[pl.ds(i * tokens, 2 * tokens)] for i in (2, 0)]
    acc = mv
    tiles = [pl.ds(t, TILE) for t in range(0, tokens, TILE)]

    def part(f, t):
        return pl.ds(f * tokens + t.start, TILE)

    passes = (0, 1, 1, 0)

    def chunk_of(k, c):
        return chunks - 1 - c if k == 2 else c

    def weight_copies(l, c, slot):
        chunk = pl.ds(c * COLS if isinstance(c, int) else pl.multiple_of(c * COLS, COLS), COLS)
        for i, (source, target) in enumerate(
            ((weights[0].at[l, :, chunk], gate_buf), (weights[1].at[l, :, chunk], up_buf), (weights[2].at[l, chunk], down_buf))
        ):
            yield pltpu.make_async_copy(source, target.at[slot], weight_sems.at[i, slot])

    def begin(k, c):
        slot = lax.rem(k * chunks + c, 2)
        for copy in weight_copies(passes[k], chunk_of(k, c), slot):
            copy.wait()

        @pl.when(c + 1 < chunks)
        def _():
            for copy in weight_copies(passes[k], chunk_of(k, c + 1), 1 - slot):
                copy.start()

        if k + 1 < len(passes):

            @pl.when(c + 1 == chunks)
            def _():
                for copy in weight_copies(passes[k + 1], chunk_of(k + 1, 0), 1 - slot):
                    copy.start()

        return slot

    def add_to_acc(t, value):
        for f in range(plan.folds):
            acc[part(f, t)] += value[:, f * COLS : (f + 1) * COLS]

    def read_acc(t):
        return jnp.concatenate([acc[part(f, t)] for f in range(plan.folds)], axis=1)

    loads = [pltpu.make_async_copy(x.at[t], x_buf.at[t], in_sems.at[i]) for i, t in enumerate(tiles)]
    load_dy = pltpu.make_async_copy(dy, dh, in_sems.at[len(tiles)])
    for copy in (*loads, *weight_copies(0, 0, 0), load_dy):
        copy.start()

    def forward(slot, t):
        gate, up = dot(a[t], gate_buf[slot]), dot(a[t], up_buf[slot])
        return dot((gate * sigmoid(gate) * up).astype(BF16), down_buf[slot])

    slot = begin(0, 0)
    for t, load in zip(tiles, loads):
        load.wait()
        a[t] = normed(x_buf[t])
        value = forward(slot, t)
        for f in range(plan.folds):
            acc[part(f, t)] = value[:, f * COLS : (f + 1) * COLS]

    @pl.loop(1, chunks - 1)
    def _(c):
        slot = begin(0, c)
        for t in tiles:
            add_to_acc(t, forward(slot, t))

    slot = begin(0, chunks - 1)
    for t in tiles:
        add = read_acc(t) + forward(slot, t)
        h = (x_buf[t].astype(F32) + add.astype(BF16).astype(F32)).astype(BF16)
        for f in range(plan.folds):
            acc[part(f, t)] = jnp.zeros((TILE, COLS), F32)
        x_buf[t] = h
        a[t] = normed(h)
    load_dy.wait()

    def hop(p, h, d):
        b = at(hops - h) if d == 0 else at(h - hops)
        if h == 0:
            source, target = own.at[p, b, d], half_landing.at[p, d]
        else:
            source, target = own.at[p, b], landing.at[p, d, h - 1]
        return pltpu.make_async_remote_copy(
            source, target, send.at[p, h, d], recv.at[p, h, d], device_id={"dp": right if d == 0 else left}, device_id_type=MESH
        )

    def advance(p, h):
        for d in (0, 1):
            if h > 0:
                hop(p, h - 1, d).wait_recv()
                b = at(hops - h) if d == 0 else at(h - hops)
                if h == 1:
                    own[p, b, d] = (own[p, b, d].astype(F32) + half_landing[p, d].astype(F32)).astype(BF16)
                else:
                    own[p, b] = (own[p, b].astype(F32) + landing[p, d, h - 2].astype(F32)).astype(BF16)
            hop(p, h, d).start()

    def finish(p):
        for d in (0, 1):
            hop(p, hops - 1, d).wait_recv()
        for half in (0, 1):
            g = own[p, me, half].astype(F32) + landing[p, 0, hops - 2, half].astype(F32) + landing[p, 1, hops - 2, half].astype(F32)
            g = g.astype(BF16)
            own[p, me, half] = g
            g = g.astype(F32)
            squares[...] += g * g

    def serve(first, last, k):
        for h in range(hops + 1):
            before = sum(at < first for at in HOPS[h])
            here = [at for at in HOPS[h] if first <= at <= last]
            if not here:
                continue
            k = jnp.int32(k)
            done = before + sum((k > at).astype(jnp.int32) for at in here)
            now = sum((k == at).astype(jnp.int32) for at in here)

            @pl.loop(done, done + now)
            def _(p, h=h):
                if h < hops:
                    advance(p, h)
                else:
                    finish(p)

    def serve_late():
        first = [sum(at < LATE for at in places) for places in HOPS]
        for h in range(hops + 1):

            @pl.loop(first[h], units)
            def _(p, h=h):
                if h < hops:
                    advance(p, h)
                else:
                    finish(p)

    def chunk_gradients(k, c, first, places):
        l = passes[k]
        slot = begin(k, c)
        if k == 1:

            @pl.when(c > 0)
            def _():
                store(c - 1).wait()

        for t in tiles:
            gate, up = dot(a[t], gate_buf[slot]), dot(a[t], up_buf[slot])
            ds = dot(dh[t], down_buf[slot], (1, 1)).astype(BF16).astype(F32)
            sig = sigmoid(gate)
            silu = gate * sig
            s_[t] = (silu * up).astype(BF16)
            du_[t] = (ds * silu).astype(BF16)
            dg_[t] = (ds * up * (sig + silu * (1.0 - sig))).astype(BF16)
        if k == 1:

            @pl.when(c + 1 < chunks)
            def _():
                store(c).start()

        serve(*places, places[0] + 3 * c)
        for half, by in ((0, dg_), (1, du_)):
            own[first + c, :, half] = dot(a[...], by[...], (0, 0)).astype(BF16).reshape(n, rows, COLS)
        serve(*places, places[0] + 3 * c + 1)
        by_down = dot(s_[...], dh[...], (0, 0)).astype(BF16)
        for g in range(COLS // plan.strip):
            group = c * (COLS // plan.strip) + g
            b, s = lax.div(group, plan.strips), lax.rem(group, plan.strips)
            i = plan.down_sub(l, s)
            for f in range(plan.folds):
                own[lax.div(i, 2), b, lax.rem(i, 2), f * plan.strip : (f + 1) * plan.strip] = by_down[
                    g * plan.strip : (g + 1) * plan.strip, f * COLS : (f + 1) * COLS
                ]
        serve(*places, places[0] + 3 * c + 2)

    pl.semaphore_wait(barrier, n - 1)
    squares[...] = jnp.zeros_like(squares)

    def store(c):
        return pltpu.make_async_copy(pairs[0], stash.at[c], stash_sems.at[2])

    def fetch(c, pair):
        return pltpu.make_async_copy(stash.at[chunk_of(2, c)], pairs[pair], stash_sems.at[pair])

    places_1 = (0, 3 * chunks - 1)
    places_in = (3 * chunks, 4 * chunks - 1)
    place_norm = 4 * chunks
    places_0 = (place_norm + 1, place_norm + 3 * chunks)

    @pl.loop(0, chunks)
    def _(c):
        chunk_gradients(1, c, plan.at["gate", 1, 0] // 2, places_1)

    @pl.loop(0, chunks)
    def _(c):
        slot = begin(2, c)

        def add(pair):
            @pl.when(c > 0)
            def _():
                fetch(c, pair).wait()

            @pl.when(c + 1 < chunks)
            def _():
                fetch(c + 1, 1 - pair).start()

            by_gate, by_up = (pairs[pair].at[pl.ds(i * tokens, tokens)] for i in (0, 1))
            for t in tiles:
                add_to_acc(t, dot(by_gate[t], gate_buf[slot], (1, 1)) + dot(by_up[t], up_buf[slot], (1, 1)))

        for pair in (0, 1):
            pl.when(lax.rem(c, 2) == pair)(lambda pair=pair: add(pair))
        serve(*places_in, places_in[0] + c)

    again = pltpu.make_async_copy(x, a, in_sems.at[0])
    again.start()
    for t in tiles:
        h, da = x_buf[t].astype(F32), read_acc(t).astype(BF16).astype(F32)
        scale = lax.rsqrt(jnp.mean(h * h, -1, keepdims=True) + 1e-6)
        by_norm = scale * da - h * (scale * scale * scale * jnp.mean(da * h, -1, keepdims=True))
        dh[t] = (dh[t].astype(F32) + by_norm.astype(BF16).astype(F32)).astype(BF16)
    again.wait()
    for t in tiles:
        a[t] = normed(a[t])

    serve(place_norm, place_norm, place_norm)

    @pl.loop(0, chunks)
    def _(c):
        chunk_gradients(3, c, plan.at["gate", 0, 0] // 2, places_0)

    w_block, m_block, v_block = flat(sdd, rows), flat(mv, rows), flat(mv, rows, len(plan.subs))
    held = len(plan.subs) * rows
    for s, (block, arrays) in enumerate(((w_block, [b.at[:, me] for b in blocks]), (m_block, moments_m), (v_block, moments_v))):
        for i in range(len(plan.subs)):
            for inside, outside in plan.views(i, block, arrays):
                pltpu.make_async_copy(outside, inside, state_sems.at[s]).start()

    serve_late()

    @pl.loop(0, units)
    def _(p):
        for h in range(hops):
            for d in (0, 1):
                hop(p, h, d).wait_send()

    folded = jnp.sum(squares[...].reshape(-1, 8, COLS), axis=0)
    sums[0] = sum(folded[:, i : i + 128] for i in range(0, COLS, 128))

    def tell(k):
        return pltpu.make_async_remote_copy(
            sums.at[0], sums.at[k], tell_send.at[k], tell_recv.at[k], device_id={"dp": at(k)}, device_id_type=MESH
        )

    for k in range(1, n):
        tell(k).start()
    for s, ref in enumerate((sdd.at[pl.ds(0, held)], mv.at[pl.ds(0, held)], mv.at[pl.ds(held, held)])):
        pltpu.make_async_copy(ref, ref, state_sems.at[s]).wait()
    for k in range(1, n):
        tell(k).wait_recv()
    total = jnp.sum(jnp.sum(sums[...], axis=0), axis=(0, 1), keepdims=True)
    factor = jnp.minimum(1.0, 0.5 * lax.rsqrt(total / count + 1e-30))
    for k in range(1, n):
        tell(k).wait_send()

    def pass_on(p, h, d):
        b = at(-h) if d == 0 else at(h)
        ref = own.at[p, b] if h < hops - 1 else own.at[p, b, d]
        return pltpu.make_async_remote_copy(
            ref, ref, send.at[p, h, d], recv.at[p, h, d], device_id={"dp": right if d == 0 else left}, device_id_type=MESH
        )

    @pl.loop(0, units)
    def _(p):
        for half in (0, 1):
            start = pl.multiple_of((2 * p + half) * rows, rows)
            here, there = pl.ds(start, rows), pl.ds(start + held, rows)
            g = own[p, me, half].astype(F32) * factor
            m = 0.9 * mv[here] + 0.1 * g
            v = 0.95 * mv[there] + 0.05 * g * g
            w = sdd[here].astype(F32)
            own[p, me, half] = (w - 0.02 * (m * lax.rsqrt(v + 1e-8) + 0.1 * w)).astype(BF16)
            mv[here] = m
            mv[there] = v
        for d in (0, 1):
            pass_on(p, 0, d).start()

    for h in range(1, hops):

        @pl.loop(0, units)
        def _(p, h=h):
            for d in (0, 1):
                pass_on(p, h - 1, d).wait_recv()
                pass_on(p, h, d).start()

    @pl.loop(0, units)
    def _(p):
        for d in (0, 1):
            pass_on(p, hops - 1, d).wait_recv()
            for h in range(hops):
                pass_on(p, h, d).wait_send()


def place_kernel(plan, own, mv, weights, new_m, new_v, sems):
    def gathered(i, part):
        return own.at[i // 2, :, i % 2, part]

    copies = []
    for i in range(len(plan.subs)):
        for s, (block, arrays, lead) in enumerate(
            (
                (gathered, weights, (EVERY,)),
                (flat(mv, plan.rows), new_m, ()),
                (flat(mv, plan.rows, len(plan.subs)), new_v, ()),
            )
        ):
            copies += [pltpu.make_async_copy(*views, sems.at[s]) for views in plan.views(i, block, arrays, lead)]
    for copy in copies:
        copy.start()
    for copy in copies:
        copy.wait()


def solution(mesh):
    n = mesh.shape["dp"]

    def step(x, dy, *arrays):
        weights, m, v = (arrays[i : i + 3] for i in (0, 3, 6))
        layers, d, ff = weights[0].shape
        tokens = x.shape[1]
        plan = Plan(n, tokens, layers, d, ff)
        blocks = [w.reshape(layers, n, -1, w.shape[-1]) for w in weights]
        count = float(sum(w.size for w in weights))
        units, rows, hops, subs = plan.units, plan.rows, plan.hops, len(plan.subs)
        anywhere, in_vmem = pl.BlockSpec(memory_space=pl.ANY), pl.BlockSpec(memory_space=pltpu.VMEM)

        def body(x, dy, *refs):
            weights, blocks, m, v = (refs[i : i + 3] for i in (0, 3, 6, 9))
            step_kernel(plan, count, x, dy, weights, blocks, m, v, *refs[12:])

        results = [pltpu.VMEM((units, n, 2, rows, COLS), BF16), pltpu.VMEM((2 * subs * rows, COLS), F32)]
        results += [jax.ShapeDtypeStruct((plan.chunks, 2 * tokens, COLS), BF16)]
        own, mv, _ = pl.pallas_call(
            body,
            out_shape=results,
            in_specs=[anywhere] * 14,
            out_specs=[in_vmem] * 2 + [anywhere],
            scratch_shapes=[pltpu.VMEM((tokens, d), BF16)] * 3
            + [
                pltpu.VMEM((4 * tokens, COLS), BF16),
                pltpu.VMEM((2, d, COLS), BF16),
                pltpu.VMEM((2, d, COLS), BF16),
                pltpu.VMEM((2, COLS, d), BF16),
                pltpu.VMEM((units, 2, rows, COLS), BF16),
                pltpu.VMEM((units, 2, hops - 1, 2, rows, COLS), BF16),
                pltpu.VMEM((rows, COLS), F32),
                pltpu.VMEM((n, 8, 128), F32),
                pltpu.SemaphoreType.DMA((tokens // TILE + 1,)),
                pltpu.SemaphoreType.DMA((3, 2)),
                pltpu.SemaphoreType.DMA((3,)),
                pltpu.SemaphoreType.DMA((3,)),
                pltpu.SemaphoreType.DMA((units, hops, 2)),
                pltpu.SemaphoreType.DMA((units, hops, 2)),
                pltpu.SemaphoreType.DMA((n,)),
                pltpu.SemaphoreType.DMA((n,)),
            ],
            compiler_params=pltpu.CompilerParams(collective_id=0, has_side_effects=True, vmem_limit_bytes=38 * 2**20),
            name="step",
        )(x[0], dy[0], *weights, *blocks, *m, *v)

        def place(*refs):
            place_kernel(plan, *refs[:2], refs[2:5], refs[5:8], refs[8:11], refs[11])

        out = pl.pallas_call(
            place,
            out_shape=[jax.ShapeDtypeStruct(t.shape, t.dtype) for t in (*blocks, *m, *v)],
            in_specs=[in_vmem] * 2,
            out_specs=[anywhere] * 9,
            scratch_shapes=[pltpu.SemaphoreType.DMA((3,))],
            compiler_params=pltpu.CompilerParams(vmem_limit_bytes=2**20),
            name="place",
        )(own, mv)
        return tuple(o.reshape(w.shape) for o, w in zip(out[:3], weights)) + tuple(out[3:])

    block = P(None, "dp", None)
    sequence = P(("rep", "dp"), None, None)
    return jax.shard_map(
        step,
        mesh=mesh,
        in_specs=(sequence, sequence, P(), P(), P()) + (block,) * 6,
        out_specs=(P("rep"),) * 3 + (P("rep", "dp", None),) * 6,
        check_vma=False,
    )
```

```python
import jax
import jax.numpy as jnp
from jax import lax
from jax.experimental import pallas as pl
from jax.experimental.pallas import tpu as pltpu
from jax.sharding import PartitionSpec as P

MESH = pl.DeviceIdType.MESH
F32, BF16 = jnp.float32, jnp.bfloat16
COLS = 256
TILE = 512
VMEM = 67_043_328
EVERY = slice(None)
LATE = 99
HOPS = (
    (1, 3, 5, 7, 10, 11, 13, 20, 20, 20, 23, 26, 30, 34, 36, 38, 42, 42, *(LATE,) * 3),
    (3, 4, 7, 9, 12, 14, 15, 21, 21, 22, 27, 30, 32, 38, 38, 42, *(LATE,) * 5),
    (5, 6, 11, 12, 14, 16, 18, 23, 24, 25, 31, 34, 37, 40, 40, *(LATE,) * 6),
    (8, 9, 15, 17, 18, 19, 20, 28, 28, 30, 36, 37, 39, 42, *(LATE,) * 7),
    (12, 13, 19, 21, 22, 23, 24, 32, 32, 34, 40, 41, *(LATE,) * 9),
)


def dot(a, b, contract=(1, 0)):
    return lax.dot_general(a, b, (((contract[0],), (contract[1],)), ((), ())), preferred_element_type=F32)


def normed(h):
    wide = h.astype(F32)
    return (wide * lax.rsqrt(jnp.mean(wide * wide, -1, keepdims=True) + 1e-6)).astype(BF16)


def sigmoid(x):
    return 0.5 * jnp.tanh(0.5 * x) + 0.5


class Plan:
    def __init__(self, n, tokens, layers, d, ff):
        self.n, self.tokens, self.layers, self.d, self.ff = n, tokens, layers, d, ff
        self.rows, self.block = d // n, ff // n
        self.folds, self.chunks = d // COLS, ff // COLS
        self.strip = self.rows // self.folds
        self.strips = self.block // self.strip
        self.hops = n // 2
        assert layers == 2 and n % 2 == 0 and d % COLS == 0 and ff % COLS == 0 and tokens % TILE == 0
        assert self.rows % (16 * self.folds) == 0 and self.block % self.strip == 0 and COLS % self.strip == 0
        self.subs, late = [], []
        for l in reversed(range(layers)):
            for c in range(self.chunks):
                self.subs += [("gate", l, c), ("up", l, c)]
            late += [("down", l, s) for s in range(self.strips)]
            even = len(late) // 2 * 2
            self.subs, late = self.subs + late[:even], late[even:]
        assert not late
        self.units = len(self.subs) // 2
        assert self.hops + 1 == len(HOPS) and all(len(h) == self.units for h in HOPS)
        self.at = {sub: i for i, sub in enumerate(self.subs)}

    def down_sub(self, l, s):
        first = self.at["down", l, 0]
        steps = [self.at["down", l, k] - self.at["down", l, k - 1] - 1 for k in range(1, self.strips)]
        place = first + s
        for k, extra in enumerate(steps, 1):
            if extra:
                place += lax.div(s + (self.strips - k), self.strips) * extra
        return place

    def views(self, i, own, arrays, lead=()):
        kind, l, k = self.subs[i]
        gate, up, down = arrays
        if kind != "down":
            yield own(i, pl.ds(0, self.rows)), (gate if kind == "gate" else up).at[(l, *lead, EVERY, pl.ds(k * COLS, COLS))]
        else:
            for f in range(self.folds):
                yield (
                    own(i, pl.ds(f * self.strip, self.strip)),
                    down.at[(l, *lead, pl.ds(k * self.strip, self.strip), pl.ds(f * COLS, COLS))],
                )


def flat(ref, rows, first=0):
    return lambda i, part: ref.at[pl.ds((first + i) * rows + part.start, part.size)]


def step_kernel(plan, count, x, dy, weights, blocks, moments_m, moments_v, own, mv, stash, *scratch):
    (x_buf, a, dh, sdd, gate_buf, up_buf, down_buf, half_landing, landing, squares, sums) = scratch[:11]
    (in_sems, weight_sems, stash_sems, state_sems, send, recv, tell_send, tell_recv) = scratch[11:]
    n, hops, units, chunks, rows, tokens = plan.n, plan.hops, plan.units, plan.chunks, plan.rows, plan.tokens
    me = lax.axis_index("dp")
    right, left = lax.rem(me + 1, n), lax.rem(me + n - 1, n)

    def at(k):
        return lax.rem(me + k + n, n)

    barrier = pltpu.get_barrier_semaphore()
    for k in range(1, n):
        pl.semaphore_signal(barrier, inc=1, device_id={"dp": at(k)}, device_id_type=MESH)

    def held(slot, i, t=None):
        start, size = (0, tokens) if t is None else (t.start, t.size)
        return sdd.at[slot, pl.ds(i * tokens + start, size)]

    acc = mv
    tiles = [pl.ds(t, TILE) for t in range(0, tokens, TILE)]

    def part(f, t):
        return pl.ds(f * tokens + t.start, TILE)

    passes = (0, 1, 1, 0)

    def chunk_of(k, c):
        return chunks - 1 - c if k == 2 else c

    def weight_copies(l, c, slot):
        chunk = pl.ds(c * COLS if isinstance(c, int) else pl.multiple_of(c * COLS, COLS), COLS)
        for i, (source, target) in enumerate(
            ((weights[0].at[l, :, chunk], gate_buf), (weights[1].at[l, :, chunk], up_buf), (weights[2].at[l, chunk], down_buf))
        ):
            yield pltpu.make_async_copy(source, target.at[slot], weight_sems.at[i, slot])

    def begin(k, c):
        slot = lax.rem(k * chunks + c, 2)
        for copy in weight_copies(passes[k], chunk_of(k, c), slot):
            copy.wait()

        @pl.when(c + 1 < chunks)
        def _():
            for copy in weight_copies(passes[k], chunk_of(k, c + 1), 1 - slot):
                copy.start()

        if k + 1 < len(passes):

            @pl.when(c + 1 == chunks)
            def _():
                for copy in weight_copies(passes[k + 1], chunk_of(k + 1, 0), 1 - slot):
                    copy.start()

        return slot

    def add_to_acc(t, value):
        for f in range(plan.folds):
            acc[part(f, t)] += value[:, f * COLS : (f + 1) * COLS]

    def read_acc(t):
        return jnp.concatenate([acc[part(f, t)] for f in range(plan.folds)], axis=1)

    loads = [pltpu.make_async_copy(x.at[t], x_buf.at[t], in_sems.at[i]) for i, t in enumerate(tiles)]
    load_dy = pltpu.make_async_copy(dy, dh, in_sems.at[len(tiles)])
    for copy in (loads[0], *weight_copies(0, 0, 0), *loads[1:]):
        copy.start()

    for f in range(plan.folds):
        acc[pl.ds(f * tokens, tokens)] = jnp.zeros((tokens, COLS), F32)
    for t, load in zip(tiles, loads):
        load.wait()
        a[t] = normed(x_buf[t])
    load_dy.start()

    def forward(c, use):
        slot = begin(0, c)
        ready = None
        for t in (*tiles, None):
            if t is not None:
                gate, up = dot(a[t], gate_buf[slot]), dot(a[t], up_buf[slot])
                after = t, (gate * sigmoid(gate) * up).astype(BF16)
            if ready is not None:
                use(ready[0], dot(ready[1], down_buf[slot]))
            ready = after

    def next_input(t, value):
        h = (x_buf[t].astype(F32) + (read_acc(t) + value).astype(BF16).astype(F32)).astype(BF16)
        for f in range(plan.folds):
            acc[part(f, t)] = jnp.zeros((TILE, COLS), F32)
        x_buf[t] = h
        a[t] = normed(h)

    @pl.loop(0, chunks - 1)
    def _(c):
        forward(c, add_to_acc)

    forward(chunks - 1, next_input)
    load_dy.wait()

    def hop(p, h, d):
        b = at(hops - h) if d == 0 else at(h - hops)
        if h == 0:
            source, target = own.at[p, b, d], half_landing.at[p, d]
        else:
            source, target = own.at[p, b], landing.at[p, d, h - 1]
        return pltpu.make_async_remote_copy(
            source, target, send.at[p, h, d], recv.at[p, h, d], device_id={"dp": right if d == 0 else left}, device_id_type=MESH
        )

    def advance(p, h):
        for d in (0, 1):
            if h > 0:
                hop(p, h - 1, d).wait_recv()
                b = at(hops - h) if d == 0 else at(h - hops)
                if h == 1:
                    own[p, b, d] = (own[p, b, d].astype(F32) + half_landing[p, d].astype(F32)).astype(BF16)
                else:
                    own[p, b] = (own[p, b].astype(F32) + landing[p, d, h - 2].astype(F32)).astype(BF16)
            hop(p, h, d).start()

    def finish(p):
        for d in (0, 1):
            hop(p, hops - 1, d).wait_recv()
        for half in (0, 1):
            g = own[p, me, half].astype(F32) + landing[p, 0, hops - 2, half].astype(F32) + landing[p, 1, hops - 2, half].astype(F32)
            g = g.astype(BF16)
            own[p, me, half] = g
            g = g.astype(F32)
            squares[...] += g * g
        for h in range(hops):
            for d in (0, 1):
                hop(p, h, d).wait_send()

    def serve(first, last, k):
        for h in range(hops + 1):
            before = sum(at < first for at in HOPS[h])
            here = [at for at in HOPS[h] if first <= at <= last]
            if not here:
                continue
            k = jnp.int32(k)
            done = before + sum((k > at).astype(jnp.int32) for at in here)
            now = sum((k == at).astype(jnp.int32) for at in here)

            @pl.loop(done, done + now)
            def _(p, h=h):
                if h < hops:
                    advance(p, h)
                else:
                    finish(p)

    def serve_late():
        first = [sum(at < LATE for at in places) for places in HOPS]
        for h in range(hops + 1):

            @pl.loop(first[h], units)
            def _(p, h=h):
                if h < hops:
                    advance(p, h)
                else:
                    finish(p)

    def hidden(slot, h):
        for t in tiles:
            gate, up = dot(a[t], gate_buf[slot]), dot(a[t], up_buf[slot])
            ds = dot(dh[t], down_buf[slot], (1, 1)).astype(BF16).astype(F32)
            sig = sigmoid(gate)
            silu = gate * sig
            held(h, 0, t)[...] = (silu * up).astype(BF16)
            held(h, 2, t)[...] = (ds * silu).astype(BF16)
            held(h, 1, t)[...] = (ds * up * (sig + silu * (1.0 - sig))).astype(BF16)

    def gate_and_up(p, h):
        for half in (0, 1):
            own[p, :, half] = dot(a[...], held(h, 1 + half)[...], (0, 0)).astype(BF16).reshape(n, rows, COLS)

    def down(l, c, h):
        by_down = dot(held(h, 0)[...], dh[...], (0, 0)).astype(BF16)
        for g in range(COLS // plan.strip):
            group = c * (COLS // plan.strip) + g
            b, s = lax.div(group, plan.strips), lax.rem(group, plan.strips)
            i = plan.down_sub(l, s)
            for f in range(plan.folds):
                own[lax.div(i, 2), b, lax.rem(i, 2), f * plan.strip : (f + 1) * plan.strip] = by_down[
                    g * plan.strip : (g + 1) * plan.strip, f * COLS : (f + 1) * COLS
                ]

    pl.semaphore_wait(barrier, n - 1)
    squares[...] = jnp.zeros_like(squares)

    def store(c, h):
        return pltpu.make_async_copy(sdd.at[h], stash.at[c], stash_sems.at[h])

    def fetch(c, h):
        return pltpu.make_async_copy(stash.at[c], sdd.at[h], stash_sems.at[h])

    late = 2 * chunks
    place_norm = late + chunks
    places_0 = place_norm + 1

    @pl.loop(0, chunks)
    def _(c):
        slot, h = begin(1, c), lax.rem(c, 2)

        @pl.when(c > 1)
        def _():
            store(c - 2, h).wait()

        hidden(slot, h)

        @pl.when(c + 1 < chunks)
        def _():
            store(c, h).start()

        serve(0, late - 1, 2 * c)
        gate_and_up(plan.at["gate", 1, 0] // 2 + c, h)
        serve(0, late - 1, 2 * c + 1)

    store(chunks - 2, (chunks - 2) % 2).wait()

    @pl.loop(0, chunks)
    def _(k):
        slot, c = begin(2, k), chunk_of(2, k)
        h = lax.rem(c, 2)

        @pl.when(k > 0)
        def _():
            fetch(c, h).wait()

        @pl.when(k + 1 < chunks)
        def _():
            fetch(chunk_of(2, k + 1), 1 - h).start()

        for t in tiles:
            add_to_acc(t, dot(held(h, 1, t)[...], gate_buf[slot], (1, 1)) + dot(held(h, 2, t)[...], up_buf[slot], (1, 1)))
        down(1, c, h)
        serve(late, place_norm - 1, late + k)

    again = pltpu.make_async_copy(x, a, in_sems.at[0])
    again.start()
    for t in tiles:
        h, da = x_buf[t].astype(F32), read_acc(t).astype(BF16).astype(F32)
        scale = lax.rsqrt(jnp.mean(h * h, -1, keepdims=True) + 1e-6)
        by_norm = scale * da - h * (scale * scale * scale * jnp.mean(da * h, -1, keepdims=True))
        dh[t] = (dh[t].astype(F32) + by_norm.astype(BF16).astype(F32)).astype(BF16)
    again.wait()
    for t in tiles:
        a[t] = normed(a[t])

    serve(place_norm, place_norm, place_norm)

    @pl.loop(0, chunks)
    def _(c):
        last = places_0 + 3 * chunks - 1
        hidden(begin(3, c), 0)
        serve(places_0, last, places_0 + 3 * c)
        gate_and_up(plan.at["gate", 0, 0] // 2 + c, 0)
        serve(places_0, last, places_0 + 3 * c + 1)
        down(0, c, 0)
        serve(places_0, last, places_0 + 3 * c + 2)

    w_rows = sdd.at[0]
    w_block, m_block, v_block = flat(w_rows, rows), flat(mv, rows), flat(mv, rows, len(plan.subs))
    mine = len(plan.subs) * rows
    for s, (block, arrays) in enumerate(((w_block, [b.at[:, me] for b in blocks]), (m_block, moments_m), (v_block, moments_v))):
        for i in range(len(plan.subs)):
            for inside, outside in plan.views(i, block, arrays):
                pltpu.make_async_copy(outside, inside, state_sems.at[s]).start()

    serve_late()

    folded = jnp.sum(squares[...].reshape(-1, 8, COLS), axis=0)
    sums[0] = sum(folded[:, i : i + 128] for i in range(0, COLS, 128))

    def tell(k):
        return pltpu.make_async_remote_copy(
            sums.at[0], sums.at[k], tell_send.at[k], tell_recv.at[k], device_id={"dp": at(k)}, device_id_type=MESH
        )

    for k in range(1, n):
        tell(k).start()
    for s, ref in enumerate((w_rows.at[pl.ds(0, mine)], mv.at[pl.ds(0, mine)], mv.at[pl.ds(mine, mine)])):
        pltpu.make_async_copy(ref, ref, state_sems.at[s]).wait()
    for k in range(1, n):
        tell(k).wait_recv()
    total = jnp.sum(jnp.sum(sums[...], axis=0), axis=(0, 1), keepdims=True)
    factor = jnp.minimum(1.0, 0.5 * lax.rsqrt(total / count + 1e-30))
    for k in range(1, n):
        tell(k).wait_send()

    def pass_on(p, h, d):
        b = at(-h) if d == 0 else at(h)
        ref = own.at[p, b] if h < hops - 1 else own.at[p, b, d]
        return pltpu.make_async_remote_copy(
            ref, ref, send.at[p, h, d], recv.at[p, h, d], device_id={"dp": right if d == 0 else left}, device_id_type=MESH
        )

    @pl.loop(0, units)
    def _(p):
        for half in (0, 1):
            start = pl.multiple_of((2 * p + half) * rows, rows)
            here, there = pl.ds(start, rows), pl.ds(start + mine, rows)
            g = own[p, me, half].astype(F32) * factor
            m = 0.9 * mv[here] + 0.1 * g
            v = 0.95 * mv[there] + 0.05 * g * g
            w = w_rows[here].astype(F32)
            own[p, me, half] = (w - 0.02 * (m * lax.rsqrt(v + 1e-8) + 0.1 * w)).astype(BF16)
            mv[here] = m
            mv[there] = v
        for d in (0, 1):
            pass_on(p, 0, d).start()

    for h in range(1, hops):

        @pl.loop(0, units)
        def _(p, h=h):
            for d in (0, 1):
                pass_on(p, h - 1, d).wait_recv()
                pass_on(p, h, d).start()

    @pl.loop(0, units)
    def _(p):
        for d in (0, 1):
            pass_on(p, hops - 1, d).wait_recv()
            for h in range(hops):
                pass_on(p, h, d).wait_send()


def place_kernel(plan, own, mv, weights, new_m, new_v, sems):
    def gathered(i, part):
        return own.at[i // 2, :, i % 2, part]

    copies = []
    for i in range(len(plan.subs)):
        for s, (block, arrays, lead) in enumerate(
            (
                (gathered, weights, (EVERY,)),
                (flat(mv, plan.rows), new_m, ()),
                (flat(mv, plan.rows, len(plan.subs)), new_v, ()),
            )
        ):
            copies += [pltpu.make_async_copy(*views, sems.at[s]) for views in plan.views(i, block, arrays, lead)]
    for copy in copies:
        copy.start()
    for copy in copies:
        copy.wait()


def solution(mesh):
    n = mesh.shape["dp"]

    def step(x, dy, *arrays):
        weights, m, v = (arrays[i : i + 3] for i in (0, 3, 6))
        layers, d, ff = weights[0].shape
        tokens = x.shape[1]
        plan = Plan(n, tokens, layers, d, ff)
        blocks = [w.reshape(layers, n, -1, w.shape[-1]) for w in weights]
        count = float(sum(w.size for w in weights))
        units, rows, hops, subs = plan.units, plan.rows, plan.hops, len(plan.subs)
        anywhere, in_vmem = pl.BlockSpec(memory_space=pl.ANY), pl.BlockSpec(memory_space=pltpu.VMEM)

        def body(x, dy, *refs):
            weights, blocks, m, v = (refs[i : i + 3] for i in (0, 3, 6, 9))
            step_kernel(plan, count, x, dy, weights, blocks, m, v, *refs[12:])

        results = [pltpu.VMEM((units, n, 2, rows, COLS), BF16), pltpu.VMEM((2 * subs * rows, COLS), F32)]
        results += [jax.ShapeDtypeStruct((plan.chunks, 3 * tokens, COLS), BF16)]
        own, mv, _ = pl.pallas_call(
            body,
            out_shape=results,
            in_specs=[anywhere] * 14,
            out_specs=[in_vmem] * 2 + [anywhere],
            scratch_shapes=[pltpu.VMEM((tokens, d), BF16)] * 3
            + [
                pltpu.VMEM((2, 3 * tokens, COLS), BF16),
                pltpu.VMEM((2, d, COLS), BF16),
                pltpu.VMEM((2, d, COLS), BF16),
                pltpu.VMEM((2, COLS, d), BF16),
                pltpu.VMEM((units, 2, rows, COLS), BF16),
                pltpu.VMEM((units, 2, hops - 1, 2, rows, COLS), BF16),
                pltpu.VMEM((rows, COLS), F32),
                pltpu.VMEM((n, 8, 128), F32),
                pltpu.SemaphoreType.DMA((tokens // TILE + 1,)),
                pltpu.SemaphoreType.DMA((3, 2)),
                pltpu.SemaphoreType.DMA((2,)),
                pltpu.SemaphoreType.DMA((3,)),
                pltpu.SemaphoreType.DMA((units, hops, 2)),
                pltpu.SemaphoreType.DMA((units, hops, 2)),
                pltpu.SemaphoreType.DMA((n,)),
                pltpu.SemaphoreType.DMA((n,)),
            ],
            compiler_params=pltpu.CompilerParams(collective_id=0, has_side_effects=True, vmem_limit_bytes=38 * 2**20),
            name="step",
        )(x[0], dy[0], *weights, *blocks, *m, *v)

        def place(*refs):
            place_kernel(plan, *refs[:2], refs[2:5], refs[5:8], refs[8:11], refs[11])

        out = pl.pallas_call(
            place,
            out_shape=[jax.ShapeDtypeStruct(t.shape, t.dtype) for t in (*blocks, *m, *v)],
            in_specs=[in_vmem] * 2,
            out_specs=[anywhere] * 9,
            scratch_shapes=[pltpu.SemaphoreType.DMA((3,))],
            compiler_params=pltpu.CompilerParams(vmem_limit_bytes=2**20),
            name="place",
        )(own, mv)
        return tuple(o.reshape(w.shape) for o, w in zip(out[:3], weights)) + tuple(out[3:])

    block = P(None, "dp", None)
    sequence = P(("rep", "dp"), None, None)
    return jax.shard_map(
        step,
        mesh=mesh,
        in_specs=(sequence, sequence, P(), P(), P()) + (block,) * 6,
        out_specs=(P("rep"),) * 3 + (P("rep", "dp", None),) * 6,
        check_vma=False,
    )
```

```python
import jax
import jax.numpy as jnp
from jax import lax
from jax.experimental import pallas as pl
from jax.experimental.pallas import tpu as pltpu
from jax.sharding import PartitionSpec as P

MESH = pl.DeviceIdType.MESH
F32, BF16 = jnp.float32, jnp.bfloat16
COLS = 256
TILE = 512
VMEM = 67_043_328
EVERY = slice(None)
LATE = 99
HOPS = (
    (1, 3, 5, 7, 10, 11, 13, 20, 20, 20, 23, 26, 30, 34, 36, 38, 42, 42, *(LATE,) * 3),
    (3, 4, 7, 9, 12, 14, 15, 21, 21, 22, 27, 30, 32, 38, 38, 42, *(LATE,) * 5),
    (5, 6, 11, 12, 14, 16, 18, 23, 24, 25, 31, 34, 37, 40, 40, *(LATE,) * 6),
    (8, 9, 15, 17, 18, 19, 20, 28, 28, 30, 36, 37, 39, 42, *(LATE,) * 7),
    (12, 13, 19, 21, 22, 23, 24, 32, 32, 34, 40, 41, *(LATE,) * 9),
)
FIRST = 2
EARLY = (4, 5)
LEAD_NS = 12_000


def dot(a, b, contract=(1, 0)):
    return lax.dot_general(a, b, (((contract[0],), (contract[1],)), ((), ())), preferred_element_type=F32)


def normed(h):
    wide = h.astype(F32)
    return (wide * lax.rsqrt(jnp.mean(wide * wide, -1, keepdims=True) + 1e-6)).astype(BF16)


def sigmoid(x):
    return 0.5 * jnp.tanh(0.5 * x) + 0.5


class Plan:
    def __init__(self, n, tokens, layers, d, ff):
        self.n, self.tokens, self.layers, self.d, self.ff = n, tokens, layers, d, ff
        self.rows, self.block = d // n, ff // n
        self.folds, self.chunks = d // COLS, ff // COLS
        self.strip = self.rows // self.folds
        self.strips = self.block // self.strip
        self.hops = n // 2
        assert layers == 2 and n % 2 == 0 and d % COLS == 0 and ff % COLS == 0 and tokens % TILE == 0
        assert self.rows % (16 * self.folds) == 0 and self.block % self.strip == 0 and COLS % self.strip == 0
        self.subs, late = [], []
        for l in reversed(range(layers)):
            for c in range(self.chunks):
                self.subs += [("gate", l, c), ("up", l, c)]
            late += [("down", l, s) for s in range(self.strips)]
            even = len(late) // 2 * 2
            self.subs, late = self.subs + late[:even], late[even:]
        assert not late
        self.units = len(self.subs) // 2
        assert self.hops + 1 == len(HOPS) and all(len(h) == self.units for h in HOPS)
        self.at = {sub: i for i, sub in enumerate(self.subs)}

    def down_sub(self, l, s):
        first = self.at["down", l, 0]
        steps = [self.at["down", l, k] - self.at["down", l, k - 1] - 1 for k in range(1, self.strips)]
        place = first + s
        for k, extra in enumerate(steps, 1):
            if extra:
                place += lax.div(s + (self.strips - k), self.strips) * extra
        return place

    def views(self, i, own, arrays, lead=()):
        kind, l, k = self.subs[i]
        gate, up, down = arrays
        if kind != "down":
            yield own(i, pl.ds(0, self.rows)), (gate if kind == "gate" else up).at[(l, *lead, EVERY, pl.ds(k * COLS, COLS))]
        else:
            for f in range(self.folds):
                yield (
                    own(i, pl.ds(f * self.strip, self.strip)),
                    down.at[(l, *lead, pl.ds(k * self.strip, self.strip), pl.ds(f * COLS, COLS))],
                )


def flat(ref, rows, first=0):
    return lambda i, part: ref.at[pl.ds((first + i) * rows + part.start, part.size)]


def step_kernel(plan, count, x, dy, weights, blocks, moments_m, moments_v, own, mv, stash, *scratch):
    (x_buf, a, dh, sdd, gate_buf, up_buf, down_buf, half_landing, landing, squares, sums, state_0, g_0) = scratch[:13]
    (in_sems, weight_sems, stash_sems, state_sems, send, recv, tell_send, tell_recv, moments_send, moments_recv, g_send, g_recv) = scratch[13:]
    n, hops, units, chunks, rows, tokens = plan.n, plan.hops, plan.units, plan.chunks, plan.rows, plan.tokens
    me = lax.axis_index("dp")
    right, left = lax.rem(me + 1, n), lax.rem(me + n - 1, n)

    def at(k):
        return lax.rem(me + k + n, n)

    barrier = pltpu.get_barrier_semaphore()
    for k in range(1, n):
        pl.semaphore_signal(barrier, inc=1, device_id={"dp": at(k)}, device_id_type=MESH)

    def held(slot, i, t=None):
        start, size = (0, tokens) if t is None else (t.start, t.size)
        return sdd.at[slot, pl.ds(i * tokens + start, size)]

    acc = mv
    tiles = [pl.ds(t, TILE) for t in range(0, tokens, TILE)]

    def part(f, t):
        return pl.ds(f * tokens + t.start, TILE)

    passes = (0, 1, 1, 0)

    def chunk_of(k, c):
        return chunks - 1 - c if k == 2 else c

    def weight_copies(l, c, slot):
        chunk = pl.ds(c * COLS if isinstance(c, int) else pl.multiple_of(c * COLS, COLS), COLS)
        for i, (source, target) in enumerate(
            ((weights[0].at[l, :, chunk], gate_buf), (weights[1].at[l, :, chunk], up_buf), (weights[2].at[l, chunk], down_buf))
        ):
            yield pltpu.make_async_copy(source, target.at[slot], weight_sems.at[i, slot])

    def begin(k, c):
        slot = lax.rem(k * chunks + c, 2)
        for copy in weight_copies(passes[k], chunk_of(k, c), slot):
            copy.wait()

        @pl.when(c + 1 < chunks)
        def _():
            for copy in weight_copies(passes[k], chunk_of(k, c + 1), 1 - slot):
                copy.start()

        if k + 1 < len(passes):

            @pl.when(c + 1 == chunks)
            def _():
                for copy in weight_copies(passes[k + 1], chunk_of(k + 1, 0), 1 - slot):
                    copy.start()

        return slot

    def add_to_acc(t, value):
        for f in range(plan.folds):
            acc[part(f, t)] += value[:, f * COLS : (f + 1) * COLS]

    def read_acc(t):
        return jnp.concatenate([acc[part(f, t)] for f in range(plan.folds)], axis=1)

    loads = [pltpu.make_async_copy(x.at[t], x_buf.at[t], in_sems.at[i]) for i, t in enumerate(tiles)]
    load_dy = pltpu.make_async_copy(dy, dh, in_sems.at[len(tiles)])
    for copy in (loads[0], *weight_copies(0, 0, 0), *loads[1:]):
        copy.start()
    for s, arrays in enumerate((moments_m, moments_v)):
        for inside, outside in plan.views(0, lambda i, part, s=s: state_0.at[me, s, part], arrays):
            pltpu.make_async_copy(outside, inside, state_sems.at[3]).start()


    def to(d):
        return {"dp": right if d == 0 else left}

    def moments(q, h, d):
        ref = state_0.at[at(-h) if d == 0 else at(h), q]
        return pltpu.make_async_remote_copy(
            ref, ref, moments_send.at[q, h, d], moments_recv.at[q, h, d], device_id=to(d), device_id_type=MESH
        )

    def move_moments(r):
        h, q = 1 + lax.div(r, 2), lax.rem(r, 2)
        for d in (0, 1):
            moments(q, h - 1, d).wait_recv()
            moments(q, h, d).start()

    def move_last_moments(q):
        moments(q, hops - 2, q).wait_recv()
        moments(q, hops - 1, q).start()

    def send_moments():
        pl.semaphore_wait(barrier, n - 1)
        pltpu.make_async_copy(state_0.at[me], state_0.at[me], state_sems.at[3]).wait()
        for q in (0, 1):
            for d in (0, 1):
                moments(q, 0, d).start()

    def forward(c, use, prepare=None):
        slot = begin(0, c)
        ready = None
        for t in (*tiles, None):
            if t is not None:
                if prepare is not None:
                    prepare(t)
                gate, up = dot(a[t], gate_buf[slot]), dot(a[t], up_buf[slot])
                after = t, (gate * sigmoid(gate) * up).astype(BF16)
            if ready is not None:
                use(ready[0], dot(ready[1], down_buf[slot]))
            ready = after

    def next_input(t, value):
        h = (x_buf[t].astype(F32) + (read_acc(t) + value).astype(BF16).astype(F32)).astype(BF16)
        x_buf[t] = h
        a[t] = normed(h)

    def first_input(t):
        a[t] = normed(x_buf[t])

    def set_acc(t, value):
        for f in range(plan.folds):
            acc[part(f, t)] = value[:, f * COLS : (f + 1) * COLS]

    for load in loads:
        load.wait()
    forward(0, set_acc, first_input)
    load_dy.start()

    @pl.loop(1, chunks - 1)
    def _(c):
        pl.when(c == FIRST)(send_moments)
        done = sum((c > at).astype(jnp.int32) for at in EARLY)
        now = sum((c == at).astype(jnp.int32) for at in EARLY)
        pl.loop(done, done + now)(move_moments)
        forward(c, add_to_acc)

    move_moments(jnp.int32(2))
    forward(chunks - 1, next_input)
    move_moments(jnp.int32(3))
    load_dy.wait()

    def hop(p, h, d):
        b = at(hops - h) if d == 0 else at(h - hops)
        if h == 0:
            source, target = own.at[p, b, d], half_landing.at[p, d]
        else:
            source, target = own.at[p, b], landing.at[p, d, h - 1]
        return pltpu.make_async_remote_copy(
            source, target, send.at[p, h, d], recv.at[p, h, d], device_id={"dp": right if d == 0 else left}, device_id_type=MESH
        )

    def advance(p, h):
        for d in (0, 1):
            if h > 0:
                hop(p, h - 1, d).wait_recv()
                b = at(hops - h) if d == 0 else at(h - hops)
                if h == 1:
                    own[p, b, d] = (own[p, b, d].astype(F32) + half_landing[p, d].astype(F32)).astype(BF16)
                else:
                    own[p, b] = (own[p, b].astype(F32) + landing[p, d, h - 2].astype(F32)).astype(BF16)
            hop(p, h, d).start()

    def finish(p):
        for d in (0, 1):
            hop(p, hops - 1, d).wait_recv()
        for half in (0, 1):
            g = own[p, me, half].astype(F32) + landing[p, 0, hops - 2, half].astype(F32) + landing[p, 1, hops - 2, half].astype(F32)
            g = g.astype(BF16)
            own[p, me, half] = g
            g = g.astype(F32)
            squares[...] += g * g
        for h in range(hops):
            for d in (0, 1):
                hop(p, h, d).wait_send()

    def serve(first, last, k):
        for h in range(hops + 1):
            before = sum(at < first for at in HOPS[h])
            here = [at for at in HOPS[h] if first <= at <= last]
            if not here:
                continue
            k = jnp.int32(k)
            done = before + sum((k > at).astype(jnp.int32) for at in here)
            now = sum((k == at).astype(jnp.int32) for at in here)

            @pl.loop(done, done + now)
            def _(p, h=h):
                if h < hops:
                    advance(p, h)
                else:
                    finish(p)

    def spread(h, d):
        ref = g_0.at[at(-h) if d == 0 else at(h)]
        return pltpu.make_async_remote_copy(ref, ref, g_send.at[h, d], g_recv.at[h, d], device_id=to(d), device_id_type=MESH)

    def spread_on(h):
        for d in (0, 1):
            if h > 0:
                spread(h - 1, d).wait_recv()
            if h < hops - 1 or d == 0:
                spread(h, d).start()

    def serve_late():
        first = [sum(at < LATE for at in places) for places in HOPS]
        for h in range(hops + 1):
            if h == hops:
                spread_on(0)

            @pl.loop(first[h], units)
            def _(p, h=h):
                if h < hops:
                    advance(p, h)
                else:
                    finish(p)

    def hidden(slot, h):
        for t in tiles:
            gate, up = dot(a[t], gate_buf[slot]), dot(a[t], up_buf[slot])
            ds = dot(dh[t], down_buf[slot], (1, 1)).astype(BF16).astype(F32)
            sig = sigmoid(gate)
            silu = gate * sig
            held(h, 0, t)[...] = (silu * up).astype(BF16)
            held(h, 2, t)[...] = (ds * silu).astype(BF16)
            held(h, 1, t)[...] = (ds * up * (sig + silu * (1.0 - sig))).astype(BF16)

    def gate_and_up(p, h):
        for half in (0, 1):
            own[p, :, half] = dot(a[...], held(h, 1 + half)[...], (0, 0)).astype(BF16).reshape(n, rows, COLS)

    def down(l, c, h):
        by_down = dot(held(h, 0)[...], dh[...], (0, 0)).astype(BF16)
        for g in range(COLS // plan.strip):
            group = c * (COLS // plan.strip) + g
            b, s = lax.div(group, plan.strips), lax.rem(group, plan.strips)
            i = plan.down_sub(l, s)
            for f in range(plan.folds):
                own[lax.div(i, 2), b, lax.rem(i, 2), f * plan.strip : (f + 1) * plan.strip] = by_down[
                    g * plan.strip : (g + 1) * plan.strip, f * COLS : (f + 1) * COLS
                ]

    squares[...] = jnp.zeros_like(squares)

    def store(c, h):
        return pltpu.make_async_copy(sdd.at[h], stash.at[c], stash_sems.at[h])

    def fetch(c, h):
        return pltpu.make_async_copy(stash.at[c], sdd.at[h], stash_sems.at[h])

    late = 2 * chunks
    place_norm = late + chunks
    places_0 = place_norm + 1

    @pl.loop(0, chunks)
    def _(c):
        slot, h = begin(1, c), lax.rem(c, 2)

        @pl.when(c > 1)
        def _():
            store(c - 2, h).wait()

        hidden(slot, h)

        @pl.when(c + 1 < chunks)
        def _():
            store(c, h).start()

        pl.when(c == 0)(lambda: move_last_moments(0))
        serve(0, late - 1, 2 * c)
        gate_and_up(plan.at["gate", 1, 0] // 2 + c, h)
        pl.when(c == 0)(lambda: move_last_moments(1))
        serve(0, late - 1, 2 * c + 1)

    store(chunks - 2, (chunks - 2) % 2).wait()
    for f in range(plan.folds):
        acc[pl.ds(f * tokens, tokens)] = jnp.zeros((tokens, COLS), F32)

    @pl.loop(0, chunks)
    def _(k):
        slot, c = begin(2, k), chunk_of(2, k)
        h = lax.rem(c, 2)

        @pl.when(k > 0)
        def _():
            fetch(c, h).wait()

        @pl.when(k + 1 < chunks)
        def _():
            fetch(chunk_of(2, k + 1), 1 - h).start()

        for t in tiles:
            add_to_acc(t, dot(held(h, 1, t)[...], gate_buf[slot], (1, 1)) + dot(held(h, 2, t)[...], up_buf[slot], (1, 1)))
        down(1, c, h)
        serve(late, place_norm - 1, late + k)

    again = pltpu.make_async_copy(x, a, in_sems.at[0])
    again.start()
    for t in tiles:
        h, da = x_buf[t].astype(F32), read_acc(t).astype(BF16).astype(F32)
        scale = lax.rsqrt(jnp.mean(h * h, -1, keepdims=True) + 1e-6)
        by_norm = scale * da - h * (scale * scale * scale * jnp.mean(da * h, -1, keepdims=True))
        dh[t] = (dh[t].astype(F32) + by_norm.astype(BF16).astype(F32)).astype(BF16)
    again.wait()
    for t in tiles:
        a[t] = normed(a[t])

    serve(place_norm, place_norm, place_norm)

    @pl.loop(0, chunks)
    def _(c):
        last = places_0 + 3 * chunks - 1
        hidden(begin(3, c), 0)
        serve(places_0, last, places_0 + 3 * c)
        gate_and_up(plan.at["gate", 0, 0] // 2 + c, 0)
        serve(places_0, last, places_0 + 3 * c + 1)
        down(0, c, 0)
        serve(places_0, last, places_0 + 3 * c + 2)

    w_rows = sdd.at[0]
    w_block, m_block, v_block = flat(w_rows, rows), flat(mv, rows), flat(mv, rows, len(plan.subs))
    mine = len(plan.subs) * rows
    for s, (block, arrays) in enumerate(((w_block, [b.at[:, me] for b in blocks]), (m_block, moments_m), (v_block, moments_v))):
        for i in range(len(plan.subs)):
            for inside, outside in plan.views(i, block, arrays):
                pltpu.make_async_copy(outside, inside, state_sems.at[s]).start()

    w_0 = sdd.at[1, pl.ds(0, plan.d)]
    _, l_0, c_0 = plan.subs[0]
    pltpu.make_async_copy(weights[0].at[l_0, :, pl.ds(c_0 * COLS, COLS)], w_0, state_sems.at[3]).start()
    g_0[me] = own[0, me, 0]

    @pl.when(lax.rem(lax.axis_index("rep"), 2) == 0)
    def _():
        pl.delay(LEAD_NS)

    serve_late()

    folded = jnp.sum(squares[...].reshape(-1, 8, COLS), axis=0)
    sums[me] = sum(folded[:, i : i + 128] for i in range(0, COLS, 128))

    def tell(k, b):
        return pltpu.make_async_remote_copy(
            sums.at[b], sums.at[b], tell_send.at[k], tell_recv.at[b], device_id={"dp": at(k)}, device_id_type=MESH
        )

    for k in range(1, n):
        tell(k, me).start()
    spread_on(1)
    for s, ref in enumerate((w_rows.at[pl.ds(0, mine)], mv.at[pl.ds(0, mine)], mv.at[pl.ds(mine, mine)], w_0)):
        pltpu.make_async_copy(ref, ref, state_sems.at[s]).wait()
    spread_on(2)
    for k in range(1, n):
        tell(k, at(k)).wait_recv()
    total = jnp.sum(jnp.sum(sums[...], axis=0), axis=(0, 1), keepdims=True)
    factor = jnp.minimum(1.0, 0.5 * lax.rsqrt(total / count + 1e-30))
    for k in range(1, n):
        tell(k, me).wait_send()

    def pass_on(p, h, d):
        b = at(-h) if d == 0 else at(h)
        if isinstance(p, int):
            ref = own.at[p, b, 1]
        else:
            ref = own.at[p, b] if h < hops - 1 else own.at[p, b, d]
        return pltpu.make_async_remote_copy(
            ref, ref, send.at[p, h, d], recv.at[p, h, d], device_id={"dp": right if d == 0 else left}, device_id_type=MESH
        )

    def pass_first_on(h):
        for d in (0, 1):
            if h > 0:
                pass_on(0, h - 1, d).wait_recv()
            if h < hops - 1 or d == 1:
                pass_on(0, h, d).start()

    def stepped(w, m, v, g):
        g = g.astype(F32) * factor
        m = 0.9 * m + 0.1 * g
        v = 0.95 * v + 0.05 * g * g
        w = w.astype(F32)
        return (w - 0.02 * (m * lax.rsqrt(v + 1e-8) + 0.1 * w)).astype(BF16), m, v

    def take_step(p, half):
        start = pl.multiple_of((2 * p + half) * rows, rows)
        here, there = pl.ds(start, rows), pl.ds(start + mine, rows)
        own[p, me, half], mv[here], mv[there] = stepped(w_rows[here], mv[here], mv[there], own[p, me, half])

    @pl.loop(1, units)
    def _(p):
        for half in (0, 1):
            take_step(p, half)
        for d in (0, 1):
            pass_on(p, 0, d).start()

    for half in (0, 1):
        take_step(0, half)
    pass_first_on(0)
    for h in range(1, hops):

        @pl.loop(1, units)
        def _(p, h=h):
            for d in (0, 1):
                pass_on(p, h - 1, d).wait_recv()
                pass_on(p, h, d).start()

        pass_first_on(h)
        if h == 1:
            spread_on(hops - 1)
        if h == 2:
            spread(hops - 1, 0).wait_recv()
            for k in range(hops):
                for d in (0, 1):
                    if k < hops - 1 or d == 0:
                        spread(k, d).wait_send()
                    for q in (0, 1):
                        if k < hops - 1 or d == q:
                            moments(q, k, d).wait_send()
                        if (k == hops - 2 and d != q) or (k == hops - 1 and d == q):
                            moments(q, k, d).wait_recv()

            @pl.loop(0, n)
            def _(b):
                w = w_0[pl.ds(pl.multiple_of(b * rows, rows), rows)]
                own[0, b, 0], _, _ = stepped(w, state_0[b, 0], state_0[b, 1], g_0[b])

    @pl.loop(1, units)
    def _(p):
        for d in (0, 1):
            pass_on(p, hops - 1, d).wait_recv()
            for h in range(hops):
                pass_on(p, h, d).wait_send()

    pass_on(0, hops - 1, 1).wait_recv()
    for h in range(hops):
        for d in (0, 1):
            if h < hops - 1 or d == 1:
                pass_on(0, h, d).wait_send()


def place_kernel(plan, own, mv, weights, new_m, new_v, sems):
    def gathered(i, part):
        return own.at[i // 2, :, i % 2, part]

    copies = []
    for i in range(len(plan.subs)):
        for s, (block, arrays, lead) in enumerate(
            (
                (gathered, weights, (EVERY,)),
                (flat(mv, plan.rows), new_m, ()),
                (flat(mv, plan.rows, len(plan.subs)), new_v, ()),
            )
        ):
            copies += [pltpu.make_async_copy(*views, sems.at[s]) for views in plan.views(i, block, arrays, lead)]
    for copy in copies:
        copy.start()
    for copy in copies:
        copy.wait()


def solution(mesh):
    n = mesh.shape["dp"]

    def step(x, dy, *arrays):
        weights, m, v = (arrays[i : i + 3] for i in (0, 3, 6))
        layers, d, ff = weights[0].shape
        tokens = x.shape[1]
        plan = Plan(n, tokens, layers, d, ff)
        blocks = [w.reshape(layers, n, -1, w.shape[-1]) for w in weights]
        count = float(sum(w.size for w in weights))
        units, rows, hops, subs = plan.units, plan.rows, plan.hops, len(plan.subs)
        anywhere, in_vmem = pl.BlockSpec(memory_space=pl.ANY), pl.BlockSpec(memory_space=pltpu.VMEM)

        def body(x, dy, *refs):
            weights, blocks, m, v = (refs[i : i + 3] for i in (0, 3, 6, 9))
            step_kernel(plan, count, x, dy, weights, blocks, m, v, *refs[12:])

        results = [pltpu.VMEM((units, n, 2, rows, COLS), BF16), pltpu.VMEM((2 * subs * rows, COLS), F32)]
        results += [jax.ShapeDtypeStruct((plan.chunks, 3 * tokens, COLS), BF16)]
        own, mv, _ = pl.pallas_call(
            body,
            out_shape=results,
            in_specs=[anywhere] * 14,
            out_specs=[in_vmem] * 2 + [anywhere],
            scratch_shapes=[pltpu.VMEM((tokens, d), BF16)] * 3
            + [
                pltpu.VMEM((2, 3 * tokens, COLS), BF16),
                pltpu.VMEM((2, d, COLS), BF16),
                pltpu.VMEM((2, d, COLS), BF16),
                pltpu.VMEM((2, COLS, d), BF16),
                pltpu.VMEM((units, 2, rows, COLS), BF16),
                pltpu.VMEM((units, 2, hops - 1, 2, rows, COLS), BF16),
                pltpu.VMEM((rows, COLS), F32),
                pltpu.VMEM((n, 8, 128), F32),
                pltpu.VMEM((n, 2, rows, COLS), F32),
                pltpu.VMEM((n, rows, COLS), BF16),
                pltpu.SemaphoreType.DMA((tokens // TILE + 1,)),
                pltpu.SemaphoreType.DMA((3, 2)),
                pltpu.SemaphoreType.DMA((2,)),
                pltpu.SemaphoreType.DMA((4,)),
                pltpu.SemaphoreType.DMA((units, hops, 2)),
                pltpu.SemaphoreType.DMA((units, hops, 2)),
                pltpu.SemaphoreType.DMA((n,)),
                pltpu.SemaphoreType.DMA((n,)),
                pltpu.SemaphoreType.DMA((2, hops, 2)),
                pltpu.SemaphoreType.DMA((2, hops, 2)),
                pltpu.SemaphoreType.DMA((hops, 2)),
                pltpu.SemaphoreType.DMA((hops, 2)),
            ],
            compiler_params=pltpu.CompilerParams(collective_id=0, has_side_effects=True, vmem_limit_bytes=40 * 2**20),
            name="step",
        )(x[0], dy[0], *weights, *blocks, *m, *v)

        def place(*refs):
            place_kernel(plan, *refs[:2], refs[2:5], refs[5:8], refs[8:11], refs[11])

        out = pl.pallas_call(
            place,
            out_shape=[jax.ShapeDtypeStruct(t.shape, t.dtype) for t in (*blocks, *m, *v)],
            in_specs=[in_vmem] * 2,
            out_specs=[anywhere] * 9,
            scratch_shapes=[pltpu.SemaphoreType.DMA((3,))],
            compiler_params=pltpu.CompilerParams(vmem_limit_bytes=2**20),
            name="place",
        )(own, mv)
        return tuple(o.reshape(w.shape) for o, w in zip(out[:3], weights)) + tuple(out[3:])

    block = P(None, "dp", None)
    sequence = P(("rep", "dp"), None, None)
    return jax.shard_map(
        step,
        mesh=mesh,
        in_specs=(sequence, sequence, P(), P(), P()) + (block,) * 6,
        out_specs=(P("rep"),) * 3 + (P("rep", "dp", None),) * 6,
        check_vma=False,
    )
```

```python
import jax
import jax.numpy as jnp
from jax import lax
from jax.experimental import pallas as pl
from jax.experimental.pallas import tpu as pltpu
from jax.sharding import PartitionSpec as P

MESH = pl.DeviceIdType.MESH
F32, BF16 = jnp.float32, jnp.bfloat16
COLS = 256
TILE = 512
VMEM = 67_043_328
EVERY = slice(None)
LATE = 99
HOPS = (
    (1, 3, 5, 7, 10, 11, 13, 20, 20, 20, 23, 26, 30, 34, 36, 38, 42, 42, *(LATE,) * 3),
    (3, 4, 7, 9, 12, 14, 15, 21, 21, 22, 27, 30, 32, 38, 38, 42, *(LATE,) * 5),
    (5, 6, 11, 12, 14, 16, 18, 23, 24, 25, 31, 34, 37, 40, 40, *(LATE,) * 6),
    (8, 9, 15, 17, 18, 19, 20, 28, 28, 30, 36, 37, 39, 42, *(LATE,) * 7),
    (12, 13, 19, 21, 22, 23, 24, 32, 32, 34, 40, 41, *(LATE,) * 9),
)
LEAD_NS = 19_000


def dot(a, b, contract=(1, 0)):
    return lax.dot_general(a, b, (((contract[0],), (contract[1],)), ((), ())), preferred_element_type=F32)


def normed(h):
    wide = h.astype(F32)
    return (wide * lax.rsqrt(jnp.mean(wide * wide, -1, keepdims=True) + 1e-6)).astype(BF16)


def sigmoid(x):
    return 0.5 * jnp.tanh(0.5 * x) + 0.5


class Plan:
    def __init__(self, n, tokens, layers, d, ff):
        self.n, self.tokens, self.layers, self.d, self.ff = n, tokens, layers, d, ff
        self.rows, self.block = d // n, ff // n
        self.folds, self.chunks = d // COLS, ff // COLS
        self.strip = self.rows // self.folds
        self.strips = self.block // self.strip
        self.hops = n // 2
        assert layers == 2 and n % 2 == 0 and d % COLS == 0 and ff % COLS == 0 and tokens % TILE == 0
        assert self.rows % (16 * self.folds) == 0 and self.block % self.strip == 0 and COLS % self.strip == 0
        self.subs, late = [], []
        for l in reversed(range(layers)):
            for c in range(self.chunks):
                self.subs += [("gate", l, c), ("up", l, c)]
            late += [("down", l, s) for s in range(self.strips)]
            even = len(late) // 2 * 2
            self.subs, late = self.subs + late[:even], late[even:]
        assert not late
        self.units = len(self.subs) // 2
        assert self.hops + 1 == len(HOPS) and all(len(h) == self.units for h in HOPS)
        self.at = {sub: i for i, sub in enumerate(self.subs)}

    def down_sub(self, l, s):
        first = self.at["down", l, 0]
        steps = [self.at["down", l, k] - self.at["down", l, k - 1] - 1 for k in range(1, self.strips)]
        place = first + s
        for k, extra in enumerate(steps, 1):
            if extra:
                place += lax.div(s + (self.strips - k), self.strips) * extra
        return place

    def views(self, i, own, arrays, lead=()):
        kind, l, k = self.subs[i]
        gate, up, down = arrays
        if kind != "down":
            yield own(i, pl.ds(0, self.rows)), (gate if kind == "gate" else up).at[(l, *lead, EVERY, pl.ds(k * COLS, COLS))]
        else:
            for f in range(self.folds):
                yield (
                    own(i, pl.ds(f * self.strip, self.strip)),
                    down.at[(l, *lead, pl.ds(k * self.strip, self.strip), pl.ds(f * COLS, COLS))],
                )


def flat(ref, rows, first=0):
    return lambda i, part: ref.at[pl.ds((first + i) * rows + part.start, part.size)]


def sums_kernel(plan, count, x, dy, weights, blocks, moments_m, moments_v, half_landing, mv, w_block, factor, stash, *scratch):
    (x_buf, a, dh, sdd, gate_buf, up_buf, down_buf, own, landing, squares, sums) = scratch[:11]
    (in_sems, weight_sems, stash_sems, state_sems, send, recv, tell_send, tell_recv) = scratch[11:]
    n, hops, units, chunks, rows, tokens = plan.n, plan.hops, plan.units, plan.chunks, plan.rows, plan.tokens
    me = lax.axis_index("dp")
    right, left = lax.rem(me + 1, n), lax.rem(me + n - 1, n)

    def at(k):
        return lax.rem(me + k + n, n)

    barrier = pltpu.get_barrier_semaphore()
    for k in range(1, n):
        pl.semaphore_signal(barrier, inc=1, device_id={"dp": at(k)}, device_id_type=MESH)

    def held(slot, i, t=None):
        start, size = (0, tokens) if t is None else (t.start, t.size)
        return sdd.at[slot, pl.ds(i * tokens + start, size)]

    acc = mv
    tiles = [pl.ds(t, TILE) for t in range(0, tokens, TILE)]

    def part(f, t):
        return pl.ds(f * tokens + t.start, TILE)

    passes = (0, 1, 1, 0)

    def chunk_of(k, c):
        return chunks - 1 - c if k == 2 else c

    def weight_copies(l, c, slot):
        chunk = pl.ds(c * COLS if isinstance(c, int) else pl.multiple_of(c * COLS, COLS), COLS)
        for i, (source, target) in enumerate(
            ((weights[0].at[l, :, chunk], gate_buf), (weights[1].at[l, :, chunk], up_buf), (weights[2].at[l, chunk], down_buf))
        ):
            yield pltpu.make_async_copy(source, target.at[slot], weight_sems.at[i, slot])

    def begin(k, c):
        slot = lax.rem(k * chunks + c, 2)
        for copy in weight_copies(passes[k], chunk_of(k, c), slot):
            copy.wait()

        @pl.when(c + 1 < chunks)
        def _():
            for copy in weight_copies(passes[k], chunk_of(k, c + 1), 1 - slot):
                copy.start()

        if k + 1 < len(passes):

            @pl.when(c + 1 == chunks)
            def _():
                for copy in weight_copies(passes[k + 1], chunk_of(k + 1, 0), 1 - slot):
                    copy.start()

        return slot

    def add_to_acc(t, value):
        for f in range(plan.folds):
            acc[part(f, t)] += value[:, f * COLS : (f + 1) * COLS]

    def read_acc(t):
        return jnp.concatenate([acc[part(f, t)] for f in range(plan.folds)], axis=1)

    loads = [pltpu.make_async_copy(x.at[t], x_buf.at[t], in_sems.at[i]) for i, t in enumerate(tiles)]
    load_dy = pltpu.make_async_copy(dy, dh, in_sems.at[len(tiles)])
    for copy in (loads[0], *weight_copies(0, 0, 0), *loads[1:]):
        copy.start()


    def forward(c, use, prepare=None):
        slot = begin(0, c)
        ready = None
        for t in (*tiles, None):
            if t is not None:
                if prepare is not None:
                    prepare(t)
                gate, up = dot(a[t], gate_buf[slot]), dot(a[t], up_buf[slot])
                after = t, (gate * sigmoid(gate) * up).astype(BF16)
            if ready is not None:
                use(ready[0], dot(ready[1], down_buf[slot]))
            ready = after

    def next_input(t, value):
        h = (x_buf[t].astype(F32) + (read_acc(t) + value).astype(BF16).astype(F32)).astype(BF16)
        x_buf[t] = h
        a[t] = normed(h)

    def first_input(t):
        a[t] = normed(x_buf[t])

    def set_acc(t, value):
        for f in range(plan.folds):
            acc[part(f, t)] = value[:, f * COLS : (f + 1) * COLS]

    for load in loads:
        load.wait()
    forward(0, set_acc, first_input)
    load_dy.start()

    @pl.loop(1, chunks - 1)
    def _(c):
        forward(c, add_to_acc)

    forward(chunks - 1, next_input)
    load_dy.wait()

    def hop(p, h, d):
        b = at(hops - h) if d == 0 else at(h - hops)
        if h == 0:
            source, target = own.at[p, b, d], half_landing.at[p, d]
        else:
            source, target = own.at[p, b], landing.at[p, d, h - 1]
        return pltpu.make_async_remote_copy(
            source, target, send.at[p, h, d], recv.at[p, h, d], device_id={"dp": right if d == 0 else left}, device_id_type=MESH
        )

    def advance(p, h):
        for d in (0, 1):
            if h > 0:
                hop(p, h - 1, d).wait_recv()
                b = at(hops - h) if d == 0 else at(h - hops)
                if h == 1:
                    own[p, b, d] = (own[p, b, d].astype(F32) + half_landing[p, d].astype(F32)).astype(BF16)
                else:
                    own[p, b] = (own[p, b].astype(F32) + landing[p, d, h - 2].astype(F32)).astype(BF16)
            hop(p, h, d).start()

    def finish(p):
        for d in (0, 1):
            hop(p, hops - 1, d).wait_recv()
        for half in (0, 1):
            g = own[p, me, half].astype(F32) + landing[p, 0, hops - 2, half].astype(F32) + landing[p, 1, hops - 2, half].astype(F32)
            g = g.astype(BF16)
            half_landing[p, half] = g
            g = g.astype(F32)
            squares[...] += g * g
        for h in range(hops):
            for d in (0, 1):
                hop(p, h, d).wait_send()

    def serve(first, last, k):
        for h in range(hops + 1):
            before = sum(at < first for at in HOPS[h])
            here = [at for at in HOPS[h] if first <= at <= last]
            if not here:
                continue
            k = jnp.int32(k)
            done = before + sum((k > at).astype(jnp.int32) for at in here)
            now = sum((k == at).astype(jnp.int32) for at in here)

            @pl.loop(done, done + now)
            def _(p, h=h):
                if h < hops:
                    advance(p, h)
                else:
                    finish(p)

    def serve_late():
        first = [sum(at < LATE for at in places) for places in HOPS]
        for h in range(hops + 1):
            @pl.loop(first[h], units)
            def _(p, h=h):
                if h < hops:
                    advance(p, h)
                else:
                    finish(p)

    def hidden(slot, h):
        for t in tiles:
            gate, up = dot(a[t], gate_buf[slot]), dot(a[t], up_buf[slot])
            ds = dot(dh[t], down_buf[slot], (1, 1)).astype(BF16).astype(F32)
            sig = sigmoid(gate)
            silu = gate * sig
            held(h, 0, t)[...] = (silu * up).astype(BF16)
            held(h, 2, t)[...] = (ds * silu).astype(BF16)
            held(h, 1, t)[...] = (ds * up * (sig + silu * (1.0 - sig))).astype(BF16)

    def gate_and_up(p, h):
        for half in (0, 1):
            own[p, :, half] = dot(a[...], held(h, 1 + half)[...], (0, 0)).astype(BF16).reshape(n, rows, COLS)

    def down(l, c, h):
        by_down = dot(held(h, 0)[...], dh[...], (0, 0)).astype(BF16)
        for g in range(COLS // plan.strip):
            group = c * (COLS // plan.strip) + g
            b, s = lax.div(group, plan.strips), lax.rem(group, plan.strips)
            i = plan.down_sub(l, s)
            for f in range(plan.folds):
                own[lax.div(i, 2), b, lax.rem(i, 2), f * plan.strip : (f + 1) * plan.strip] = by_down[
                    g * plan.strip : (g + 1) * plan.strip, f * COLS : (f + 1) * COLS
                ]

    pl.semaphore_wait(barrier, n - 1)
    squares[...] = jnp.zeros_like(squares)

    def store(c, h):
        return pltpu.make_async_copy(sdd.at[h], stash.at[c], stash_sems.at[h])

    def fetch(c, h):
        return pltpu.make_async_copy(stash.at[c], sdd.at[h], stash_sems.at[h])

    late = 2 * chunks
    place_norm = late + chunks
    places_0 = place_norm + 1

    @pl.loop(0, chunks)
    def _(c):
        slot, h = begin(1, c), lax.rem(c, 2)

        @pl.when(c > 1)
        def _():
            store(c - 2, h).wait()

        hidden(slot, h)

        @pl.when(c + 1 < chunks)
        def _():
            store(c, h).start()

        serve(0, late - 1, 2 * c)
        gate_and_up(plan.at["gate", 1, 0] // 2 + c, h)
        serve(0, late - 1, 2 * c + 1)

    store(chunks - 2, (chunks - 2) % 2).wait()
    for f in range(plan.folds):
        acc[pl.ds(f * tokens, tokens)] = jnp.zeros((tokens, COLS), F32)

    @pl.loop(0, chunks)
    def _(k):
        slot, c = begin(2, k), chunk_of(2, k)
        h = lax.rem(c, 2)

        @pl.when(k > 0)
        def _():
            fetch(c, h).wait()

        @pl.when(k + 1 < chunks)
        def _():
            fetch(chunk_of(2, k + 1), 1 - h).start()

        for t in tiles:
            add_to_acc(t, dot(held(h, 1, t)[...], gate_buf[slot], (1, 1)) + dot(held(h, 2, t)[...], up_buf[slot], (1, 1)))
        down(1, c, h)
        serve(late, place_norm - 1, late + k)

    again = pltpu.make_async_copy(x, a, in_sems.at[0])
    again.start()
    for t in tiles:
        h, da = x_buf[t].astype(F32), read_acc(t).astype(BF16).astype(F32)
        scale = lax.rsqrt(jnp.mean(h * h, -1, keepdims=True) + 1e-6)
        by_norm = scale * da - h * (scale * scale * scale * jnp.mean(da * h, -1, keepdims=True))
        dh[t] = (dh[t].astype(F32) + by_norm.astype(BF16).astype(F32)).astype(BF16)
    again.wait()
    for t in tiles:
        a[t] = normed(a[t])

    serve(place_norm, place_norm, place_norm)

    @pl.loop(0, chunks)
    def _(c):
        last = places_0 + 3 * chunks - 1
        hidden(begin(3, c), 0)
        serve(places_0, last, places_0 + 3 * c)
        gate_and_up(plan.at["gate", 0, 0] // 2 + c, 0)
        serve(places_0, last, places_0 + 3 * c + 1)
        down(0, c, 0)
        serve(places_0, last, places_0 + 3 * c + 2)

    own_blocks = (
        (flat(mv, rows), moments_m),
        (flat(mv, rows, len(plan.subs)), moments_v),
        (flat(w_block, rows), [b.at[:, me] for b in blocks]),
    )
    for s, (block, arrays) in enumerate(own_blocks):
        for i in range(len(plan.subs)):
            for inside, outside in plan.views(i, block, arrays):
                pltpu.make_async_copy(outside, inside, state_sems.at[s]).start()

    @pl.when(lax.rem(lax.axis_index("rep"), 2) == 0)
    def _():
        pl.delay(LEAD_NS)

    serve_late()

    folded = jnp.sum(squares[...].reshape(-1, 8, COLS), axis=0)
    sums[me] = sum(folded[:, i : i + 128] for i in range(0, COLS, 128))

    def tell(k, b):
        return pltpu.make_async_remote_copy(
            sums.at[b], sums.at[b], tell_send.at[k], tell_recv.at[b], device_id={"dp": at(k)}, device_id_type=MESH
        )

    for k in range(1, n):
        tell(k, me).start()
    mine = len(plan.subs) * rows
    for s, ref in enumerate((mv.at[pl.ds(0, mine)], mv.at[pl.ds(mine, mine)], w_block)):
        pltpu.make_async_copy(ref, ref, state_sems.at[s]).wait()
    for k in range(1, n):
        tell(k, at(k)).wait_recv()
    total = jnp.sum(jnp.sum(sums[...], axis=0), axis=(0, 1), keepdims=True)
    factor[...] = jnp.broadcast_to(jnp.minimum(1.0, 0.5 * lax.rsqrt(total / count + 1e-30)), factor.shape)
    for k in range(1, n):
        tell(k, me).wait_send()


def update_kernel(plan, g, mv, w, factor, new_w, moments_m, moments_v, new_mv, out_sems):
    rows, subs = plan.rows, len(plan.subs)
    scale = factor[0:1, 0:1]
    copies = []
    for first in range(0, plan.units, 3):

        @pl.loop(first, first + 3)
        def _(p):
            for half in (0, 1):
                start = pl.multiple_of((2 * p + half) * rows, rows)
                here, there = pl.ds(start, rows), pl.ds(start + subs * rows, rows)
                by = g[p, half].astype(F32) * scale
                m = 0.9 * mv[here] + 0.1 * by
                v = 0.95 * mv[there] + 0.05 * by * by
                old = w[here].astype(F32)
                new_w[p, half] = (old - 0.02 * (m * lax.rsqrt(v + 1e-8) + 0.1 * old)).astype(BF16)
                new_mv[here] = m
                new_mv[there] = v

        for i in range(2 * first, 2 * (first + 3)):
            for s, (shift, arrays) in enumerate(((0, moments_m), (subs, moments_v))):
                for views in plan.views(i, flat(new_mv, rows, shift), arrays):
                    copies.append(pltpu.make_async_copy(*views, out_sems.at[s]))
                    copies[-1].start()
    for copy in copies:
        copy.wait()


def gather_kernel(plan, new_w, own, send, recv):
    n, hops, units = plan.n, plan.hops, plan.units
    me = lax.axis_index("dp")
    right, left = lax.rem(me + 1, n), lax.rem(me + n - 1, n)
    barrier = pltpu.get_barrier_semaphore()
    for to in (right, left):
        pl.semaphore_signal(barrier, inc=1, device_id={"dp": to}, device_id_type=MESH)
    pl.semaphore_wait(barrier, 2)

    def pass_on(p, h, d):
        b = lax.rem(me - h + n, n) if d == 0 else lax.rem(me + h, n)
        target = own.at[p, b] if h < hops - 1 else own.at[p, b, d]
        return pltpu.make_async_remote_copy(
            new_w.at[p] if h == 0 else target,
            target,
            send.at[p, h, d],
            recv.at[p, h, d],
            device_id={"dp": right if d == 0 else left},
            device_id_type=MESH,
        )

    @pl.loop(0, units)
    def _(p):
        for d in (0, 1):
            pass_on(p, 0, d).start()

    @pl.loop(0, units)
    def _(p):
        own[p, me] = new_w[p]

    for h in range(1, hops):

        @pl.loop(0, units)
        def _(p, h=h):
            for d in (0, 1):
                pass_on(p, h - 1, d).wait_recv()
                pass_on(p, h, d).start()

    @pl.loop(0, units)
    def _(p):
        for d in (0, 1):
            pass_on(p, hops - 1, d).wait_recv()
            for h in range(hops):
                pass_on(p, h, d).wait_send()


def place_kernel(plan, own, weights, sem):
    def gathered(i, part):
        return own.at[i // 2, :, i % 2, part]

    copies = [pltpu.make_async_copy(*views, sem) for i in range(len(plan.subs)) for views in plan.views(i, gathered, weights, (EVERY,))]
    for copy in copies:
        copy.start()
    for copy in copies:
        copy.wait()


def solution(mesh):
    n = mesh.shape["dp"]

    def step(x, dy, *arrays):
        weights, m, v = (arrays[i : i + 3] for i in (0, 3, 6))
        layers, d, ff = weights[0].shape
        tokens = x.shape[1]
        plan = Plan(n, tokens, layers, d, ff)
        blocks = [w.reshape(layers, n, -1, w.shape[-1]) for w in weights]
        count = float(sum(w.size for w in weights))
        units, rows, hops, subs = plan.units, plan.rows, plan.hops, len(plan.subs)
        anywhere, in_vmem = pl.BlockSpec(memory_space=pl.ANY), pl.BlockSpec(memory_space=pltpu.VMEM)

        assert units % 3 == 0
        unit = (units, 2, rows, COLS)
        flat_moments = pltpu.VMEM((2 * subs * rows, COLS), F32)

        def call(kernel, name, results, operands, spaces, out_spaces, scratch, limit, remote=None):
            params = {} if remote is None else {"collective_id": remote, "has_side_effects": True}
            return pl.pallas_call(
                kernel,
                out_shape=results,
                in_specs=spaces,
                out_specs=out_spaces,
                scratch_shapes=scratch,
                compiler_params=pltpu.CompilerParams(vmem_limit_bytes=limit * 2**20, **params),
                name=name,
            )(*operands)

        def sums(x, dy, *refs):
            sums_kernel(plan, count, x, dy, *(refs[i : i + 3] for i in (0, 3, 6, 9)), *refs[12:])

        g, mv, w_block, factor, _ = call(
            sums,
            "sums",
            [pltpu.VMEM(unit, BF16), flat_moments, pltpu.VMEM((subs * rows, COLS), BF16), pltpu.VMEM((8, 128), F32)]
            + [jax.ShapeDtypeStruct((plan.chunks, 3 * tokens, COLS), BF16)],
            (x[0], dy[0], *weights, *blocks, *m, *v),
            [anywhere] * 14,
            [in_vmem] * 4 + [anywhere],
            [pltpu.VMEM((tokens, d), BF16)] * 3
            + [
                pltpu.VMEM((2, 3 * tokens, COLS), BF16),
                pltpu.VMEM((2, d, COLS), BF16),
                pltpu.VMEM((2, d, COLS), BF16),
                pltpu.VMEM((2, COLS, d), BF16),
                pltpu.VMEM((units, n, 2, rows, COLS), BF16),
                pltpu.VMEM((units, 2, hops - 1, 2, rows, COLS), BF16),
                pltpu.VMEM((rows, COLS), F32),
                pltpu.VMEM((n, 8, 128), F32),
                pltpu.SemaphoreType.DMA((tokens // TILE + 1,)),
                pltpu.SemaphoreType.DMA((3, 2)),
                pltpu.SemaphoreType.DMA((2,)),
                pltpu.SemaphoreType.DMA((3,)),
                pltpu.SemaphoreType.DMA((units, hops, 2)),
                pltpu.SemaphoreType.DMA((units, hops, 2)),
                pltpu.SemaphoreType.DMA((n,)),
                pltpu.SemaphoreType.DMA((n,)),
            ],
            51,
            remote=0,
        )

        def update(*refs):
            update_kernel(plan, *refs[:5], refs[5:8], refs[8:11], *refs[11:])

        new_w, *new_moments = call(
            update,
            "update",
            [pltpu.VMEM(unit, BF16)] + [jax.ShapeDtypeStruct(t.shape, t.dtype) for t in (*m, *v)],
            (g, mv, w_block, factor),
            [in_vmem] * 4,
            [in_vmem] + [anywhere] * 6,
            [flat_moments, pltpu.SemaphoreType.DMA((2,))],
            10,
        )

        def gather(*refs):
            gather_kernel(plan, *refs)

        own = call(
            gather,
            "gather",
            pltpu.VMEM((units, n, 2, rows, COLS), BF16),
            (new_w,),
            [in_vmem],
            in_vmem,
            [pltpu.SemaphoreType.DMA((units, hops, 2)), pltpu.SemaphoreType.DMA((units, hops, 2))],
            2,
            remote=1,
        )

        def place(own, *refs):
            place_kernel(plan, own, refs[:3], refs[3])

        new_weights = call(
            place,
            "place",
            [jax.ShapeDtypeStruct(t.shape, t.dtype) for t in blocks],
            (own,),
            [in_vmem],
            [anywhere] * 3,
            [pltpu.SemaphoreType.DMA],
            1,
        )
        return tuple(o.reshape(w.shape) for o, w in zip(new_weights, weights)) + tuple(new_moments)

    block = P(None, "dp", None)
    sequence = P(("rep", "dp"), None, None)
    return jax.shard_map(
        step,
        mesh=mesh,
        in_specs=(sequence, sequence, P(), P(), P()) + (block,) * 6,
        out_specs=(P("rep"),) * 3 + (P("rep", "dp", None),) * 6,
        check_vma=False,
    )
```

```python
import jax
import jax.numpy as jnp
from jax import lax
from jax.experimental import pallas as pl
from jax.experimental.pallas import tpu as pltpu
from jax.sharding import PartitionSpec as P

MESH = pl.DeviceIdType.MESH
F32, BF16 = jnp.float32, jnp.bfloat16
COLS = 256
TILE = 512
VMEM = 67_043_328
EVERY = slice(None)
LATE = 99
HOPS = (
    (1, 3, 5, 7, 10, 11, 13, 20, 20, 20, 23, 26, 30, 34, 36, 38, 42, 42, *(LATE,) * 3),
    (3, 4, 7, 9, 12, 14, 15, 21, 21, 22, 27, 30, 32, 38, 38, 42, *(LATE,) * 5),
    (5, 6, 11, 12, 14, 16, 18, 23, 24, 25, 31, 34, 37, 40, 40, *(LATE,) * 6),
    (8, 9, 15, 17, 18, 19, 20, 28, 28, 30, 36, 37, 39, 42, *(LATE,) * 7),
    (12, 13, 19, 21, 22, 23, 24, 32, 32, 34, 40, 41, *(LATE,) * 9),
)
LEAD_NS = 21_000


def dot(a, b, contract=(1, 0)):
    return lax.dot_general(a, b, (((contract[0],), (contract[1],)), ((), ())), preferred_element_type=F32)


def normed(h):
    wide = h.astype(F32)
    return (wide * lax.rsqrt(jnp.mean(wide * wide, -1, keepdims=True) + 1e-6)).astype(BF16)


def sigmoid(x):
    return 0.5 * jnp.tanh(0.5 * x) + 0.5


class Plan:
    def __init__(self, n, tokens, layers, d, ff):
        self.n, self.tokens, self.layers, self.d, self.ff = n, tokens, layers, d, ff
        self.rows, self.block = d // n, ff // n
        self.folds, self.chunks = d // COLS, ff // COLS
        self.strip = self.rows // self.folds
        self.strips = self.block // self.strip
        self.hops = n // 2
        assert layers == 2 and n % 2 == 0 and d % COLS == 0 and ff % COLS == 0 and tokens % TILE == 0
        assert self.rows % (16 * self.folds) == 0 and self.block % self.strip == 0 and COLS % self.strip == 0
        self.subs, late = [], []
        for l in reversed(range(layers)):
            for c in range(self.chunks):
                self.subs += [("gate", l, c), ("up", l, c)]
            late += [("down", l, s) for s in range(self.strips)]
            even = len(late) // 2 * 2
            self.subs, late = self.subs + late[:even], late[even:]
        assert not late
        self.units = len(self.subs) // 2
        assert self.hops + 1 == len(HOPS) and all(len(h) == self.units for h in HOPS)
        self.at = {sub: i for i, sub in enumerate(self.subs)}

    def down_sub(self, l, s):
        first = self.at["down", l, 0]
        steps = [self.at["down", l, k] - self.at["down", l, k - 1] - 1 for k in range(1, self.strips)]
        place = first + s
        for k, extra in enumerate(steps, 1):
            if extra:
                place += lax.div(s + (self.strips - k), self.strips) * extra
        return place

    def views(self, i, own, arrays, lead=()):
        kind, l, k = self.subs[i]
        gate, up, down = arrays
        if kind != "down":
            yield own(i, pl.ds(0, self.rows)), (gate if kind == "gate" else up).at[(l, *lead, EVERY, pl.ds(k * COLS, COLS))]
        else:
            for f in range(self.folds):
                yield (
                    own(i, pl.ds(f * self.strip, self.strip)),
                    down.at[(l, *lead, pl.ds(k * self.strip, self.strip), pl.ds(f * COLS, COLS))],
                )


def flat(ref, rows, first=0):
    return lambda i, part: ref.at[pl.ds((first + i) * rows + part.start, part.size)]


def sums_kernel(plan, count, x, dy, weights, blocks, moments_m, moments_v, half_landing, mv, w_block, factor, stash, *scratch):
    (x_buf, a, dh, sdd, gate_buf, up_buf, down_buf, own, landing, squares, sums) = scratch[:11]
    (in_sems, weight_sems, stash_sems, state_sems, send, recv, tell_send, tell_recv) = scratch[11:]
    n, hops, units, chunks, rows, tokens = plan.n, plan.hops, plan.units, plan.chunks, plan.rows, plan.tokens
    me = lax.axis_index("dp")
    right, left = lax.rem(me + 1, n), lax.rem(me + n - 1, n)

    def at(k):
        return lax.rem(me + k + n, n)

    barrier = pltpu.get_barrier_semaphore()
    for k in range(1, n):
        pl.semaphore_signal(barrier, inc=1, device_id={"dp": at(k)}, device_id_type=MESH)

    def held(slot, i, t=None):
        start, size = (0, tokens) if t is None else (t.start, t.size)
        return sdd.at[slot, pl.ds(i * tokens + start, size)]

    acc = mv
    tiles = [pl.ds(t, TILE) for t in range(0, tokens, TILE)]

    def part(f, t):
        return pl.ds(f * tokens + t.start, TILE)

    passes = (0, 1, 1, 0)

    def chunk_of(k, c):
        return chunks - 1 - c if k == 2 else c

    def weight_copies(l, c, slot):
        chunk = pl.ds(c * COLS if isinstance(c, int) else pl.multiple_of(c * COLS, COLS), COLS)
        for i, (source, target) in enumerate(
            ((weights[0].at[l, :, chunk], gate_buf), (weights[1].at[l, :, chunk], up_buf), (weights[2].at[l, chunk], down_buf))
        ):
            yield pltpu.make_async_copy(source, target.at[slot], weight_sems.at[i, slot])

    def begin(k, c):
        slot = lax.rem(k * chunks + c, 2)
        for copy in weight_copies(passes[k], chunk_of(k, c), slot):
            copy.wait()

        @pl.when(c + 1 < chunks)
        def _():
            for copy in weight_copies(passes[k], chunk_of(k, c + 1), 1 - slot):
                copy.start()

        if k + 1 < len(passes):

            @pl.when(c + 1 == chunks)
            def _():
                for copy in weight_copies(passes[k + 1], chunk_of(k + 1, 0), 1 - slot):
                    copy.start()

        return slot

    def add_to_acc(t, value):
        for f in range(plan.folds):
            acc[part(f, t)] += value[:, f * COLS : (f + 1) * COLS]

    def read_acc(t):
        return jnp.concatenate([acc[part(f, t)] for f in range(plan.folds)], axis=1)

    loads = [pltpu.make_async_copy(x.at[t], x_buf.at[t], in_sems.at[i]) for i, t in enumerate(tiles)]
    load_dy = pltpu.make_async_copy(dy, dh, in_sems.at[len(tiles)])
    for copy in (loads[0], *weight_copies(0, 0, 0), *loads[1:]):
        copy.start()


    def forward(c, use, prepare=None):
        slot = begin(0, c)
        ready = None
        for t in (*tiles, None):
            if t is not None:
                if prepare is not None:
                    prepare(t)
                gate, up = dot(a[t], gate_buf[slot]), dot(a[t], up_buf[slot])
                after = t, (gate * sigmoid(gate) * up).astype(BF16)
            if ready is not None:
                use(ready[0], dot(ready[1], down_buf[slot]))
            ready = after

    def next_input(t, value):
        h = (x_buf[t].astype(F32) + (read_acc(t) + value).astype(BF16).astype(F32)).astype(BF16)
        x_buf[t] = h
        a[t] = normed(h)

    def first_input(t):
        a[t] = normed(x_buf[t])

    def set_acc(t, value):
        for f in range(plan.folds):
            acc[part(f, t)] = value[:, f * COLS : (f + 1) * COLS]

    for load in loads:
        load.wait()
    forward(0, set_acc, first_input)
    load_dy.start()

    @pl.loop(1, chunks - 1)
    def _(c):
        forward(c, add_to_acc)

    forward(chunks - 1, next_input)
    load_dy.wait()

    def hop(p, h, d):
        b = at(hops - h) if d == 0 else at(h - hops)
        if h == 0:
            source, target = own.at[p, b, d], half_landing.at[p, d]
        else:
            source, target = own.at[p, b], landing.at[p, d, h - 1]
        return pltpu.make_async_remote_copy(
            source, target, send.at[p, h, d], recv.at[p, h, d], device_id={"dp": right if d == 0 else left}, device_id_type=MESH
        )

    def advance(p, h):
        for d in (0, 1):
            if h > 0:
                hop(p, h - 1, d).wait_recv()
                b = at(hops - h) if d == 0 else at(h - hops)
                if h == 1:
                    own[p, b, d] = (own[p, b, d].astype(F32) + half_landing[p, d].astype(F32)).astype(BF16)
                else:
                    own[p, b] = (own[p, b].astype(F32) + landing[p, d, h - 2].astype(F32)).astype(BF16)
            hop(p, h, d).start()

    def finish(p):
        for d in (0, 1):
            hop(p, hops - 1, d).wait_recv()
        for half in (0, 1):
            g = own[p, me, half].astype(F32) + landing[p, 0, hops - 2, half].astype(F32) + landing[p, 1, hops - 2, half].astype(F32)
            g = g.astype(BF16)
            half_landing[p, half] = g
            g = g.astype(F32)
            squares[...] += g * g
        for h in range(hops):
            for d in (0, 1):
                hop(p, h, d).wait_send()

    def serve(first, last, k):
        for h in range(hops + 1):
            before = sum(at < first for at in HOPS[h])
            here = [at for at in HOPS[h] if first <= at <= last]
            if not here:
                continue
            k = jnp.int32(k)
            done = before + sum((k > at).astype(jnp.int32) for at in here)
            now = sum((k == at).astype(jnp.int32) for at in here)

            @pl.loop(done, done + now)
            def _(p, h=h):
                if h < hops:
                    advance(p, h)
                else:
                    finish(p)

    def serve_late():
        first = [sum(at < LATE for at in places) for places in HOPS]
        for h in range(hops + 1):
            @pl.loop(first[h], units)
            def _(p, h=h):
                if h < hops:
                    advance(p, h)
                else:
                    finish(p)

    def hidden(slot, h):
        for t in tiles:
            gate, up = dot(a[t], gate_buf[slot]), dot(a[t], up_buf[slot])
            ds = dot(dh[t], down_buf[slot], (1, 1)).astype(BF16).astype(F32)
            sig = sigmoid(gate)
            silu = gate * sig
            held(h, 0, t)[...] = (silu * up).astype(BF16)
            held(h, 2, t)[...] = (ds * silu).astype(BF16)
            held(h, 1, t)[...] = (ds * up * (sig + silu * (1.0 - sig))).astype(BF16)

    def gate_and_up(p, h):
        for half in (0, 1):
            own[p, :, half] = dot(a[...], held(h, 1 + half)[...], (0, 0)).astype(BF16).reshape(n, rows, COLS)

    def down(l, c, h):
        by_down = dot(held(h, 0)[...], dh[...], (0, 0)).astype(BF16)
        for g in range(COLS // plan.strip):
            group = c * (COLS // plan.strip) + g
            b, s = lax.div(group, plan.strips), lax.rem(group, plan.strips)
            i = plan.down_sub(l, s)
            for f in range(plan.folds):
                own[lax.div(i, 2), b, lax.rem(i, 2), f * plan.strip : (f + 1) * plan.strip] = by_down[
                    g * plan.strip : (g + 1) * plan.strip, f * COLS : (f + 1) * COLS
                ]

    pl.semaphore_wait(barrier, n - 1)
    squares[...] = jnp.zeros_like(squares)

    def store(c, h):
        return pltpu.make_async_copy(sdd.at[h], stash.at[c], stash_sems.at[h])

    def fetch(c, h):
        return pltpu.make_async_copy(stash.at[c], sdd.at[h], stash_sems.at[h])

    late = 2 * chunks
    place_norm = late + chunks
    places_0 = place_norm + 1

    @pl.loop(0, chunks)
    def _(c):
        slot, h = begin(1, c), lax.rem(c, 2)

        @pl.when(c > 1)
        def _():
            store(c - 2, h).wait()

        hidden(slot, h)

        @pl.when(c + 1 < chunks)
        def _():
            store(c, h).start()

        serve(0, late - 1, 2 * c)
        gate_and_up(plan.at["gate", 1, 0] // 2 + c, h)
        serve(0, late - 1, 2 * c + 1)

    store(chunks - 2, (chunks - 2) % 2).wait()
    for f in range(plan.folds):
        acc[pl.ds(f * tokens, tokens)] = jnp.zeros((tokens, COLS), F32)

    @pl.loop(0, chunks)
    def _(k):
        slot, c = begin(2, k), chunk_of(2, k)
        h = lax.rem(c, 2)

        @pl.when(k > 0)
        def _():
            fetch(c, h).wait()

        @pl.when(k + 1 < chunks)
        def _():
            fetch(chunk_of(2, k + 1), 1 - h).start()

        for t in tiles:
            add_to_acc(t, dot(held(h, 1, t)[...], gate_buf[slot], (1, 1)) + dot(held(h, 2, t)[...], up_buf[slot], (1, 1)))
        down(1, c, h)
        serve(late, place_norm - 1, late + k)

    again = pltpu.make_async_copy(x, a, in_sems.at[0])
    again.start()
    for t in tiles:
        h, da = x_buf[t].astype(F32), read_acc(t).astype(BF16).astype(F32)
        scale = lax.rsqrt(jnp.mean(h * h, -1, keepdims=True) + 1e-6)
        by_norm = scale * da - h * (scale * scale * scale * jnp.mean(da * h, -1, keepdims=True))
        dh[t] = (dh[t].astype(F32) + by_norm.astype(BF16).astype(F32)).astype(BF16)
    again.wait()
    for t in tiles:
        a[t] = normed(a[t])

    serve(place_norm, place_norm, place_norm)

    @pl.loop(0, chunks)
    def _(c):
        last = places_0 + 3 * chunks - 1
        hidden(begin(3, c), 0)
        serve(places_0, last, places_0 + 3 * c)
        gate_and_up(plan.at["gate", 0, 0] // 2 + c, 0)
        serve(places_0, last, places_0 + 3 * c + 1)
        down(0, c, 0)
        serve(places_0, last, places_0 + 3 * c + 2)

    own_blocks = (
        (flat(mv, rows), moments_m),
        (flat(mv, rows, len(plan.subs)), moments_v),
        (flat(w_block, rows), [b.at[:, me] for b in blocks]),
    )
    for s, (block, arrays) in enumerate(own_blocks):
        for i in range(len(plan.subs)):
            for inside, outside in plan.views(i, block, arrays):
                pltpu.make_async_copy(outside, inside, state_sems.at[s]).start()

    @pl.when(lax.rem(lax.axis_index("rep"), 2) == 0)
    def _():
        pl.delay(LEAD_NS)

    serve_late()

    folded = jnp.sum(squares[...].reshape(-1, 8, COLS), axis=0)
    sums[me] = sum(folded[:, i : i + 128] for i in range(0, COLS, 128))

    def tell(k, b):
        return pltpu.make_async_remote_copy(
            sums.at[b], sums.at[b], tell_send.at[k], tell_recv.at[b], device_id={"dp": at(k)}, device_id_type=MESH
        )

    for k in range(1, n):
        tell(k, me).start()
    mine = len(plan.subs) * rows
    for s, ref in enumerate((mv.at[pl.ds(0, mine)], mv.at[pl.ds(mine, mine)], w_block)):
        pltpu.make_async_copy(ref, ref, state_sems.at[s]).wait()
    for k in range(1, n):
        tell(k, at(k)).wait_recv()
    total = jnp.sum(jnp.sum(sums[...], axis=0), axis=(0, 1), keepdims=True)
    factor[...] = jnp.broadcast_to(jnp.minimum(1.0, 0.5 * lax.rsqrt(total / count + 1e-30)), factor.shape)
    for k in range(1, n):
        tell(k, me).wait_send()


def update_kernel(plan, g, mv, w, factor, new_w, moments_m, moments_v, new_mv, out_sems):
    rows, subs = plan.rows, len(plan.subs)
    scale = factor[0:1, 0:1]
    copies = []
    for first in range(0, plan.units, 3):

        @pl.loop(first, first + 3)
        def _(p):
            for half in (0, 1):
                start = pl.multiple_of((2 * p + half) * rows, rows)
                here, there = pl.ds(start, rows), pl.ds(start + subs * rows, rows)
                by = g[p, half].astype(F32) * scale
                m = 0.9 * mv[here] + 0.1 * by
                v = 0.95 * mv[there] + 0.05 * by * by
                old = w[here].astype(F32)
                new_w[p, half] = (old - 0.02 * (m * lax.rsqrt(v + 1e-8) + 0.1 * old)).astype(BF16)
                new_mv[here] = m
                new_mv[there] = v

        for i in range(2 * first, 2 * (first + 3)):
            for s, (shift, arrays) in enumerate(((0, moments_m), (subs, moments_v))):
                for views in plan.views(i, flat(new_mv, rows, shift), arrays):
                    copies.append(pltpu.make_async_copy(*views, out_sems.at[s]))
                    copies[-1].start()
    for copy in copies:
        copy.wait()


def gather_kernel(plan, new_w, own, send, recv):
    n, hops, units = plan.n, plan.hops, plan.units
    me = lax.axis_index("dp")
    right, left = lax.rem(me + 1, n), lax.rem(me + n - 1, n)
    barrier = pltpu.get_barrier_semaphore()
    for to in (right, left):
        pl.semaphore_signal(barrier, inc=1, device_id={"dp": to}, device_id_type=MESH)
    pl.semaphore_wait(barrier, 2)

    def pass_on(p, h, d):
        b = lax.rem(me - h + n, n) if d == 0 else lax.rem(me + h, n)
        target = own.at[p, b] if h < hops - 1 else own.at[p, b, d]
        return pltpu.make_async_remote_copy(
            new_w.at[p] if h == 0 else target,
            target,
            send.at[p, h, d],
            recv.at[p, h, d],
            device_id={"dp": right if d == 0 else left},
            device_id_type=MESH,
        )

    @pl.loop(0, units)
    def _(p):
        for d in (0, 1):
            pass_on(p, 0, d).start()

    @pl.loop(0, units)
    def _(p):
        own[p, me] = new_w[p]

    for h in range(1, hops):

        @pl.loop(0, units)
        def _(p, h=h):
            for d in (0, 1):
                pass_on(p, h - 1, d).wait_recv()
                pass_on(p, h, d).start()

    @pl.loop(0, units)
    def _(p):
        for d in (0, 1):
            pass_on(p, hops - 1, d).wait_recv()
            for h in range(hops):
                pass_on(p, h, d).wait_send()


def place_kernel(plan, own, weights, sem):
    def gathered(i, part):
        return own.at[i // 2, :, i % 2, part]

    copies = [pltpu.make_async_copy(*views, sem) for i in range(len(plan.subs)) for views in plan.views(i, gathered, weights, (EVERY,))]
    for copy in copies:
        copy.start()
    for copy in copies:
        copy.wait()


def solution(mesh):
    n = mesh.shape["dp"]

    def step(x, dy, *arrays):
        weights, m, v = (arrays[i : i + 3] for i in (0, 3, 6))
        layers, d, ff = weights[0].shape
        tokens = x.shape[1]
        plan = Plan(n, tokens, layers, d, ff)
        blocks = [w.reshape(layers, n, -1, w.shape[-1]) for w in weights]
        count = float(sum(w.size for w in weights))
        units, rows, hops, subs = plan.units, plan.rows, plan.hops, len(plan.subs)
        anywhere, in_vmem = pl.BlockSpec(memory_space=pl.ANY), pl.BlockSpec(memory_space=pltpu.VMEM)

        assert units % 3 == 0
        unit = (units, 2, rows, COLS)
        flat_moments = pltpu.VMEM((2 * subs * rows, COLS), F32)

        def call(kernel, name, results, operands, spaces, out_spaces, scratch, limit, remote=None):
            params = {} if remote is None else {"collective_id": remote, "has_side_effects": True}
            return pl.pallas_call(
                kernel,
                out_shape=results,
                in_specs=spaces,
                out_specs=out_spaces,
                scratch_shapes=scratch,
                compiler_params=pltpu.CompilerParams(vmem_limit_bytes=limit * 2**20, **params),
                name=name,
            )(*operands)

        def sums(x, dy, *refs):
            sums_kernel(plan, count, x, dy, *(refs[i : i + 3] for i in (0, 3, 6, 9)), *refs[12:])

        g, mv, w_block, factor, _ = call(
            sums,
            "sums",
            [pltpu.VMEM(unit, BF16), flat_moments, pltpu.VMEM((subs * rows, COLS), BF16), pltpu.VMEM((8, 128), F32)]
            + [jax.ShapeDtypeStruct((plan.chunks, 3 * tokens, COLS), BF16)],
            (x[0], dy[0], *weights, *blocks, *m, *v),
            [anywhere] * 14,
            [in_vmem] * 4 + [anywhere],
            [pltpu.VMEM((tokens, d), BF16)] * 3
            + [
                pltpu.VMEM((2, 3 * tokens, COLS), BF16),
                pltpu.VMEM((2, d, COLS), BF16),
                pltpu.VMEM((2, d, COLS), BF16),
                pltpu.VMEM((2, COLS, d), BF16),
                pltpu.VMEM((units, n, 2, rows, COLS), BF16),
                pltpu.VMEM((units, 2, hops - 1, 2, rows, COLS), BF16),
                pltpu.VMEM((rows, COLS), F32),
                pltpu.VMEM((n, 8, 128), F32),
                pltpu.SemaphoreType.DMA((tokens // TILE + 1,)),
                pltpu.SemaphoreType.DMA((3, 2)),
                pltpu.SemaphoreType.DMA((2,)),
                pltpu.SemaphoreType.DMA((3,)),
                pltpu.SemaphoreType.DMA((units, hops, 2)),
                pltpu.SemaphoreType.DMA((units, hops, 2)),
                pltpu.SemaphoreType.DMA((n,)),
                pltpu.SemaphoreType.DMA((n,)),
            ],
            51,
            remote=0,
        )

        def update(*refs):
            update_kernel(plan, *refs[:5], refs[5:8], refs[8:11], *refs[11:])

        new_w, *new_moments = call(
            update,
            "update",
            [pltpu.VMEM(unit, BF16)] + [jax.ShapeDtypeStruct(t.shape, t.dtype) for t in (*m, *v)],
            (g, mv, w_block, factor),
            [in_vmem] * 4,
            [in_vmem] + [anywhere] * 6,
            [flat_moments, pltpu.SemaphoreType.DMA((2,))],
            10,
        )

        def gather(*refs):
            gather_kernel(plan, *refs)

        own = call(
            gather,
            "gather",
            pltpu.VMEM((units, n, 2, rows, COLS), BF16),
            (new_w,),
            [in_vmem],
            in_vmem,
            [pltpu.SemaphoreType.DMA((units, hops, 2)), pltpu.SemaphoreType.DMA((units, hops, 2))],
            2,
            remote=1,
        )

        def place(own, *refs):
            place_kernel(plan, own, refs[:3], refs[3])

        new_weights = call(
            place,
            "place",
            [jax.ShapeDtypeStruct(t.shape, t.dtype) for t in blocks],
            (own,),
            [in_vmem],
            [anywhere] * 3,
            [pltpu.SemaphoreType.DMA],
            1,
        )
        return tuple(o.reshape(w.shape) for o, w in zip(new_weights, weights)) + tuple(new_moments)

    block = P(None, "dp", None)
    sequence = P(("rep", "dp"), None, None)
    return jax.shard_map(
        step,
        mesh=mesh,
        in_specs=(sequence, sequence, P(), P(), P()) + (block,) * 6,
        out_specs=(P("rep"),) * 3 + (P("rep", "dp", None),) * 6,
        check_vma=False,
    )
```
